16 devices in a mesh: prob: 4 (over z, y), feat: 4 (over x, core).
Axes of the slice: x: 2, y: 2, z: 2, core: 2. Of those that a mesh axis runs over, the one named last changes fastest.
Arguments:
- design: bfloat16 [65536, 2048], P('prob', 'feat'), parts along dimension 0
- coef_init: float32 [8192, 8], P(('prob', 'feat')), parts along dimension 0
- targets: float32 [65536, 8], P('prob'), parts along dimension 0
- step_sizes: float32 [8192], P(('prob', 'feat')), parts along dimension 0
Outputs:
- output 1: float32 [8192, 8], P(('prob', 'feat')), parts along dimension 0
- output 2: float32 [65536, 8], P('prob'), parts along dimension 0
There are 4 independent parts. The reference program is written for one: setup_inputs(seed, part) draws one part's arguments, and reference() takes and returns one part's arrays. A program takes and returns all parts, laid end to end along the dimension named above; each array names one.
All inputs are finite; a program needn't handle non-finite values.
Results may differ from the reference program's by a relative error of at most 0.0057789.
Values are sent between devices in bfloat16 or wider.
A program may use at most 1 GiB of HBM per device.

```python
import jax
import jax.numpy as jnp
from jax import lax

SAMPLES = 16384
FEAT_DEV = 512
GROUP_SIZE = 4
TARGETS = 8
SWEEPS = 6
FACTORS = 4

FEATURES = FEAT_DEV * GROUP_SIZE
COMBINE_WEIGHT = 0.8
LASSO_WEIGHT = 0.3 * GROUP_SIZE / FEATURES ** 0.5


def setup_inputs(seed: int = 0, part: int = 0) -> dict:
    part_key = jax.random.fold_in(jax.random.key(seed), part)
    draw_keys = jax.random.split(part_key, 9)
    factor_rows = jax.random.normal(draw_keys[0], (SAMPLES, FACTORS), jnp.float32)
    loadings = jax.random.normal(draw_keys[1], (FACTORS, FEATURES), jnp.float32) * (0.5 / FEAT_DEV) ** 0.5

    def draw_block(block_index):
        noise_x = jax.random.normal(jax.random.fold_in(draw_keys[2], block_index), (SAMPLES, FEAT_DEV), jnp.float32)
        load_block = lax.dynamic_slice_in_dim(loadings, block_index * FEAT_DEV, FEAT_DEV, 1)
        x_block = (jnp.dot(factor_rows, load_block) + noise_x).astype(jnp.bfloat16)
        col_sq = jnp.sum(jnp.square(x_block.astype(jnp.float32)), axis=0)
        return x_block, col_sq

    x_blocks, col_sq = lax.map(draw_block, jnp.arange(GROUP_SIZE))
    design = jnp.transpose(x_blocks, (1, 0, 2)).reshape(SAMPLES, FEATURES)
    step_scale = jax.random.uniform(draw_keys[3], (FEATURES,), jnp.float32, 0.5, 1.0)
    step_sizes = step_scale * SAMPLES / (GROUP_SIZE * col_sq.reshape(FEATURES))
    support = jax.random.bernoulli(draw_keys[4], 0.125, (FEATURES, TARGETS)).astype(jnp.float32)
    true_weights = jax.random.normal(draw_keys[5], (FEATURES, TARGETS), jnp.float32) * support * (4.0 / FEATURES) ** 0.5
    factor_weights = jax.random.normal(draw_keys[6], (FACTORS, TARGETS), jnp.float32) * FACTORS ** -0.5
    noise_y = jax.random.normal(draw_keys[7], (SAMPLES, TARGETS), jnp.float32)
    signal = jnp.dot(design, true_weights.astype(jnp.bfloat16), preferred_element_type=jnp.float32)
    targets = jnp.dot(factor_rows, factor_weights) + signal + 0.5 * noise_y
    coef_init = jax.random.normal(draw_keys[8], (FEATURES, TARGETS), jnp.float32) * FEATURES ** -0.5
    return {'design': design, 'coef_init': coef_init, 'targets': targets, 'step_sizes': step_sizes}


def reference(design, coef_init, targets, step_sizes):
    x_blocks = jnp.transpose(design.reshape(SAMPLES, GROUP_SIZE, FEAT_DEV), (1, 0, 2))
    step_col = step_sizes[:, None]
    thresholds = step_col * LASSO_WEIGHT

    def block_sum(values):
        value_blocks = values.astype(jnp.bfloat16).reshape(GROUP_SIZE, FEAT_DEV, TARGETS)

        def add_block(running, operands):
            x_block, v_block = operands
            product = jnp.dot(x_block, v_block, preferred_element_type=jnp.float32).astype(jnp.bfloat16)
            return running + product.astype(jnp.float32), None

        running, _ = lax.scan(add_block, jnp.zeros((SAMPLES, TARGETS), jnp.float32), (x_blocks, value_blocks))
        return running

    residual = targets - block_sum(coef_init)

    def sweep(carry, _):
        weights, residual = carry
        gradient = lax.dot_general(design, residual.astype(jnp.bfloat16), (((0,), (0,)), ((), ())), preferred_element_type=jnp.float32) / SAMPLES
        stepped = weights + step_col * gradient
        shrunk = jnp.sign(stepped) * jnp.maximum(jnp.abs(stepped) - thresholds, 0.0)
        change = shrunk - weights
        weights = weights + COMBINE_WEIGHT * change
        residual = residual - COMBINE_WEIGHT * block_sum(change)
        return (weights, residual), None

    (weights, residual), _ = lax.scan(sweep, (coef_init, residual), None, length=SWEEPS)
    return (weights, residual)
```

```python
import functools

import jax
import jax.numpy as jnp
from jax import lax
from jax.experimental import pallas as pl
from jax.experimental.pallas import tpu as pltpu
from jax.sharding import PartitionSpec as P

SWEEPS = 6
COMBINE_WEIGHT = 0.8
EXPLICIT = False
LAG = 3
TILE = 256
MESH = pl.DeviceIdType.MESH
OWN, PARTNER, CROSS, RELAYED = 0, 1, 2, 3


def chunk_list(samples):
    size = samples // 16
    return [(i * size, size) for i in range(16)]


def kernel(chunks, lasso_weight, samples, *refs):
    (x_hbm, w0_ref, y_hbm, eta_ref, w_out, r_out, xv, rv, ubuf, wv, dwv, gv, x_sem, y_sem, out_sem,
     own_send, cross_send, relay_send, own_recv, cross_recv, relay_recv) = refs
    count = len(chunks)
    targets, features = w0_ref.shape
    depth_tiles = features // TILE
    me = lax.axis_index('feat')
    partner = me + 1 - 2 * lax.rem(me, 2)
    cross = 3 - me

    def rows_of(c):
        start, size = chunks[c]
        return pl.ds(start, size)

    def x_copy(c):
        return pltpu.make_async_copy(x_hbm.at[rows_of(c)], xv.at[rows_of(c)], x_sem.at[c])

    def remote(par, c, src, dst, peer, send_sem, recv_sem):
        return pltpu.make_async_remote_copy(
            src_ref=ubuf.at[par, src, :, rows_of(c)], dst_ref=ubuf.at[par, dst, :, rows_of(c)],
            send_sem=send_sem.at[par, c], recv_sem=recv_sem.at[par, c], device_id={'feat': peer}, device_id_type=MESH)

    def own_copy(par, c):
        return remote(par, c, OWN, PARTNER, partner, own_send, own_recv)

    def cross_copy(par, c):
        return remote(par, c, OWN, CROSS, cross, cross_send, cross_recv)

    def relay_copy(par, c):
        return remote(par, c, CROSS, RELAYED, partner, relay_send, relay_recv)

    def body(*accs):
        forward_acc = [accs[:len(accs) // 2 - 1], accs[len(accs) // 2:-1]]
        gradient_acc = [accs[len(accs) // 2 - 1], accs[-1]]

        def tiles_of(c):
            start, size = chunks[c]
            return [start + i * TILE for i in range(size // TILE)]

        def acc_of(c, i):
            half = len(forward_acc[0]) // 2
            return forward_acc[i % 2][(c % 2) * half + i // 2]

        def issue_forward(c):
            if not EXPLICIT:
                return
            change = [dwv[:, kt * TILE:(kt + 1) * TILE] for kt in range(depth_tiles)]
            for i, row in enumerate(tiles_of(c)):
                for kt in range(depth_tiles):
                    pltpu.matmul_push_rhs(xv[pl.ds(row, TILE), pl.ds(kt * TILE, TILE)], staging_register=kt % 2, mxu_index=i % 2, transpose=True)
                    pltpu.matmul_acc_lhs(acc_of(c, i), change[kt], load_staged_rhs=kt % 2)

        def collect_forward(par, c):
            for i, row in enumerate(tiles_of(c)):
                if EXPLICIT:
                    product = pltpu.matmul_pop(acc_of(c, i))
                else:
                    product = lax.dot_general(dwv[...].astype(jnp.bfloat16), xv[pl.ds(row, TILE), :], (((1,), (1,)), ((), ())), preferred_element_type=jnp.float32)
                ubuf[par, OWN, :, pl.ds(row, TILE)] = product.astype(jnp.bfloat16)

        def issue_gradient(c):
            for row in tiles_of(c):
                lhs = rv[:, pl.ds(row, TILE)].astype(jnp.bfloat16).astype(jnp.float32)
                for q in range(depth_tiles):
                    x_tile = xv[pl.ds(row, TILE), pl.ds(q * TILE, TILE)]
                    if EXPLICIT:
                        pltpu.matmul_push_rhs(x_tile, staging_register=(row // TILE) % 2, mxu_index=q)
                        pltpu.matmul_acc_lhs(gradient_acc[q], lhs, load_staged_rhs=(row // TILE) % 2)
                    else:
                        gv[:, pl.ds(q * TILE, TILE)] += jnp.dot(lhs.astype(jnp.bfloat16), x_tile, preferred_element_type=jnp.float32)

        def update_weights():
            for q in range(depth_tiles):
                cols = pl.ds(q * TILE, TILE)
                if EXPLICIT:
                    gradient = pltpu.matmul_pop(gradient_acc[q])
                else:
                    gradient = gv[:, cols]
                    gv[:, cols] = jnp.zeros_like(gradient)
                eta = jnp.broadcast_to(eta_ref[:, cols], (targets, TILE))
                threshold = eta * lasso_weight
                weights = wv[:, cols]
                stepped = weights + eta * (gradient * (1.0 / samples))
                shrunk = jnp.where(stepped > threshold, stepped - threshold, jnp.where(stepped < -threshold, stepped + threshold, 0.0))
                change = shrunk - weights
                wv[:, cols] = weights + COMBINE_WEIGHT * change
                dwv[:, cols] = change.astype(jnp.bfloat16).astype(jnp.float32)

        def wait_sends(par):
            for c in range(count):
                own_copy(par, c).wait_send()
                cross_copy(par, c).wait_send()
                relay_copy(par, c).wait_send()

        def phase(par, first=False, last=False):
            def send(c):
                collect_forward(par, c)
                cross_copy(par, c).start()
                own_copy(par, c).start()

            for c in range(count):
                if first:
                    x_copy(c).wait()
                issue_forward(c)
                if c > 0:
                    send(c - 1)
                if c == count // 2 and not first:
                    wait_sends(1 - par)
            send(count - 1)
            if first:
                pltpu.make_async_copy(y_hbm, rv, y_sem).wait()
            for step in range(count + LAG):
                if step < count:
                    cross_copy(par, step).wait_recv()
                    relay_copy(par, step).start()
                c = step - LAG
                if c < 0:
                    continue
                own_copy(par, c).wait_recv()
                relay_copy(par, c).wait_recv()
                for row in tiles_of(c):
                    cols = pl.ds(row, TILE)
                    u = [ubuf[par, slot, :, cols].astype(jnp.float32) for slot in range(4)]
                    total = (u[OWN] + u[PARTNER]) + (u[CROSS] + u[RELAYED])
                    rv[:, cols] = rv[:, cols] - (total if first else COMBINE_WEIGHT * total)
                if last:
                    pltpu.make_async_copy(rv.at[:, rows_of(c)], r_out.at[:, rows_of(c)], out_sem.at[c]).start()
                else:
                    issue_gradient(c)
            if not last:
                update_weights()

        phase(0, first=True)

        def sweep(s, carry):
            phase(lax.rem(s, 2))
            return carry

        lax.fori_loop(1, SWEEPS, sweep, 0)
        phase(SWEEPS % 2, last=True)
        w_out[...] = wv[...]
        wait_sends(SWEEPS % 2)
        for c in range(count):
            pltpu.make_async_copy(rv.at[:, rows_of(c)], r_out.at[:, rows_of(c)], out_sem.at[c]).wait()

    for c in range(count):
        x_copy(c).start()
        if c == 0:
            pltpu.make_async_copy(y_hbm, rv, y_sem).start()
    barrier = pltpu.get_barrier_semaphore()
    for peer in (partner, cross):
        pl.semaphore_signal(barrier, inc=1, device_id={'feat': peer}, device_id_type=MESH)
    wv[...] = w0_ref[...]
    dwv[...] = w0_ref[...].astype(jnp.bfloat16).astype(jnp.float32)
    if not EXPLICIT:
        gv[...] = jnp.zeros_like(gv)
    pl.semaphore_wait(barrier, 2)
    if EXPLICIT:
        per_mxu = 2 * max(size for _, size in chunks) // TILE // 2
        specs = [pltpu.ACC(q)((targets, TILE), jnp.float32) for q in range(2) for _ in range(per_mxu + 1)]
        pl.run_scoped(body, *specs)
    else:
        body(*[None] * 4)


def solution(mesh):
    group_size = mesh.shape['feat']

    def local_run(x_local, coef_local, targets_local, step_local):
        samples, local_features = x_local.shape
        targets = coef_local.shape[1]
        features = local_features * group_size
        lasso_weight = 0.3 * group_size / features ** 0.5
        chunks = chunk_list(samples)
        count = len(chunks)
        any_spec = pl.BlockSpec(memory_space=pl.ANY)
        vmem_spec = pl.BlockSpec(memory_space=pltpu.VMEM)
        dma = pltpu.SemaphoreType.DMA
        w_t, r_t = pl.pallas_call(
            functools.partial(kernel, chunks, lasso_weight, samples),
            out_shape=(jax.ShapeDtypeStruct((targets, local_features), jnp.float32), jax.ShapeDtypeStruct((targets, samples), jnp.float32)),
            in_specs=[any_spec, vmem_spec, any_spec, vmem_spec],
            out_specs=(vmem_spec, any_spec),
            scratch_shapes=[
                pltpu.VMEM((samples, local_features), jnp.bfloat16),
                pltpu.VMEM((targets, samples), jnp.float32),
                pltpu.VMEM((2, 4, targets, samples), jnp.bfloat16),
                pltpu.VMEM((targets, local_features), jnp.float32),
                pltpu.VMEM((targets, local_features), jnp.float32),
                pltpu.VMEM((targets, local_features), jnp.float32),
                dma((count,)), dma, dma((count,)),
                dma((2, count)), dma((2, count)), dma((2, count)), dma((2, count)), dma((2, count)), dma((2, count)),
            ],
            compiler_params=pltpu.CompilerParams(collective_id=0, has_side_effects=True, vmem_limit_bytes=60 * 1024 * 1024),
            name='block_lasso',
        )(x_local, coef_local.T, targets_local.T, step_local[None, :])
        return w_t.T, r_t.T

    return jax.shard_map(local_run, mesh=mesh, in_specs=(P('prob', 'feat'), P(('prob', 'feat'), None), P('prob', None), P(('prob', 'feat'))), out_specs=(P(('prob', 'feat'), None), P('prob', None)), check_vma=False)
```

```python
import functools

import jax
import jax.numpy as jnp
from jax import lax
from jax.experimental import pallas as pl
from jax.experimental.pallas import tpu as pltpu
from jax.sharding import PartitionSpec as P

SWEEPS = 6
COMBINE_WEIGHT = 0.8
LAG = 3
TILE = 256
MESH = pl.DeviceIdType.MESH
OWN, PARTNER, CROSS, RELAYED = 0, 1, 2, 3


def chunk_list(samples):
    size = samples // 16
    return [(i * size, size) for i in range(16)]


def kernel(chunks, lasso_weight, samples, *refs):
    (x_hbm, w0_ref, y_hbm, eta_ref, wv, rv, xv, xt, ubuf, dwv, x_sem, y_sem,
     own_send, cross_send, relay_send, own_recv, cross_recv, relay_recv) = refs
    count = len(chunks)
    targets = w0_ref.shape[0]
    me = lax.axis_index('feat')
    partner = me + 1 - 2 * lax.rem(me, 2)
    cross = 3 - me

    def rows_of(c):
        start, size = chunks[c]
        return pl.ds(start, size)

    def tiles_of(c):
        start, size = chunks[c]
        return range(start // TILE, (start + size) // TILE)

    def x_copy(c):
        return pltpu.make_async_copy(x_hbm.at[rows_of(c)], xv.at[rows_of(c)], x_sem.at[c])

    def remote(par, c, src, dst, peer, send_sem, recv_sem):
        return pltpu.make_async_remote_copy(
            src_ref=ubuf.at[par, src, :, rows_of(c)], dst_ref=ubuf.at[par, dst, :, rows_of(c)],
            send_sem=send_sem.at[par, c], recv_sem=recv_sem.at[par, c], device_id={'feat': peer}, device_id_type=MESH)

    def own_copy(par, c):
        return remote(par, c, OWN, PARTNER, partner, own_send, own_recv)

    def cross_copy(par, c):
        return remote(par, c, OWN, CROSS, cross, cross_send, cross_recv)

    def relay_copy(par, c):
        return remote(par, c, CROSS, RELAYED, partner, relay_send, relay_recv)

    def forward(par, c, first):
        change = dwv[...]
        for t in tiles_of(c):
            rows = pl.ds(t * TILE, TILE)
            if first:
                x_t = xv[rows, :].T
                xt[t] = x_t
            else:
                x_t = xt[t]
            product = jnp.dot(change, x_t, preferred_element_type=jnp.float32)
            ubuf[par, OWN, :, rows] = product.astype(jnp.bfloat16)

    def update_weights(gradient):
        eta = jnp.broadcast_to(eta_ref[...], gradient.shape)
        threshold = eta * lasso_weight
        weights = wv[...]
        stepped = weights + eta * (gradient * (1.0 / samples))
        shrunk = jnp.where(stepped > threshold, stepped - threshold, jnp.where(stepped < -threshold, stepped + threshold, 0.0))
        change = shrunk - weights
        wv[...] = weights + COMBINE_WEIGHT * change
        dwv[...] = change.astype(jnp.bfloat16)

    def wait_sends(par):
        for c in range(count):
            own_copy(par, c).wait_send()
            cross_copy(par, c).wait_send()
            relay_copy(par, c).wait_send()

    def phase(par, first=False, last=False):
        for c in range(count):
            if first:
                x_copy(c).wait()
            forward(par, c, first)
            if c == count // 2 and not first:
                wait_sends(1 - par)
            cross_copy(par, c).start()
            own_copy(par, c).start()
        if first:
            pltpu.make_async_copy(y_hbm, rv, y_sem).wait()
        gradient = None
        for step in range(count + LAG):
            if step < count:
                cross_copy(par, step).wait_recv()
                relay_copy(par, step).start()
            c = step - LAG
            if c < 0:
                continue
            own_copy(par, c).wait_recv()
            relay_copy(par, c).wait_recv()
            rows = rows_of(c)
            u = [ubuf[par, slot, :, rows].astype(jnp.float32) for slot in range(4)]
            total = (u[OWN] + u[PARTNER]) + (u[CROSS] + u[RELAYED])
            residual = rv[:, rows] - (total if first else COMBINE_WEIGHT * total)
            rv[:, rows] = residual
            if not last:
                part = jnp.dot(residual.astype(jnp.bfloat16), xv[rows, :], preferred_element_type=jnp.float32)
                gradient = part if gradient is None else gradient + part
        if not last:
            update_weights(gradient)

    for c in range(count):
        x_copy(c).start()
        if c == 0:
            pltpu.make_async_copy(y_hbm, rv, y_sem).start()
    barrier = pltpu.get_barrier_semaphore()
    for peer in (partner, cross):
        pl.semaphore_signal(barrier, inc=1, device_id={'feat': peer}, device_id_type=MESH)
    wv[...] = w0_ref[...]
    dwv[...] = w0_ref[...].astype(jnp.bfloat16)
    pl.semaphore_wait(barrier, 2)

    phase(0, first=True)

    def sweep(s, carry):
        phase(lax.rem(s, 2))
        return carry

    lax.fori_loop(1, SWEEPS, sweep, 0)
    phase(SWEEPS % 2, last=True)
    wait_sends(SWEEPS % 2)


def solution(mesh):
    group_size = mesh.shape['feat']

    def local_run(x_local, coef_local, targets_local, step_local):
        samples, local_features = x_local.shape
        targets = coef_local.shape[1]
        features = local_features * group_size
        lasso_weight = 0.3 * group_size / features ** 0.5
        chunks = chunk_list(samples)
        count = len(chunks)
        any_spec = pl.BlockSpec(memory_space=pl.ANY)
        vmem_spec = pl.BlockSpec(memory_space=pltpu.VMEM)
        dma = pltpu.SemaphoreType.DMA
        w_t, r_t = pl.pallas_call(
            functools.partial(kernel, chunks, lasso_weight, samples),
            out_shape=(pltpu.VMEM((targets, local_features), jnp.float32), pltpu.VMEM((targets, samples), jnp.float32)),
            in_specs=[pl.BlockSpec(memory_space=pltpu.HBM), vmem_spec, pl.BlockSpec(memory_space=pltpu.HBM), vmem_spec],
            out_specs=(vmem_spec, vmem_spec),
            scratch_shapes=[
                pltpu.VMEM((samples, local_features), jnp.bfloat16),
                pltpu.VMEM((samples // TILE, local_features, TILE), jnp.bfloat16),
                pltpu.VMEM((2, 4, targets, samples), jnp.bfloat16),
                pltpu.VMEM((targets, local_features), jnp.bfloat16),
                dma((count,)), dma,
                dma((2, count)), dma((2, count)), dma((2, count)), dma((2, count)), dma((2, count)), dma((2, count)),
            ],
            compiler_params=pltpu.CompilerParams(collective_id=0, has_side_effects=True, vmem_limit_bytes=60 * 1024 * 1024),
            name='block_lasso',
        )(x_local, coef_local.T, targets_local.T, step_local[None, :])
        return w_t.T, r_t.T

    return jax.shard_map(local_run, mesh=mesh, in_specs=(P('prob', 'feat'), P(('prob', 'feat'), None), P('prob', None), P(('prob', 'feat'))), out_specs=(P(('prob', 'feat'), None), P('prob', None)), check_vma=False)
```

```python
import functools

import jax
import jax.numpy as jnp
from jax import lax
from jax.experimental import pallas as pl
from jax.experimental.pallas import tpu as pltpu
from jax.sharding import PartitionSpec as P

SWEEPS = 6
COMBINE_WEIGHT = 0.8
LAG = 3
TILE = 256
MESH = pl.DeviceIdType.MESH
OWN, PARTNER, CROSS, RELAYED = 0, 1, 2, 3


def chunk_list(samples):
    size = samples // 16
    return [(i * size, size) for i in range(16)]


def kernel(chunks, lasso_weight, samples, *refs):
    (x_hbm, w0_ref, y_hbm, eta_ref, wv, rv, xv, xt, ubuf, dwv, x_sem, y_sem,
     own_send, cross_send, relay_send, own_recv, cross_recv, relay_recv) = refs
    count = len(chunks)
    targets = w0_ref.shape[0]
    me = lax.axis_index('feat')
    partner = me + 1 - 2 * lax.rem(me, 2)
    cross = lax.rem(me + 2, 4)

    def rows_of(c):
        start, size = chunks[c]
        return pl.ds(start, size)

    def tiles_of(c):
        start, size = chunks[c]
        return range(start // TILE, (start + size) // TILE)

    def x_copy(c):
        return pltpu.make_async_copy(x_hbm.at[rows_of(c)], xv.at[rows_of(c)], x_sem.at[c])

    def remote(par, c, src, dst, peer, send_sem, recv_sem):
        return pltpu.make_async_remote_copy(
            src_ref=ubuf.at[par, src, :, rows_of(c)], dst_ref=ubuf.at[par, dst, :, rows_of(c)],
            send_sem=send_sem.at[par, c], recv_sem=recv_sem.at[par, c], device_id={'feat': peer}, device_id_type=MESH)

    def own_copy(par, c):
        return remote(par, c, OWN, PARTNER, partner, own_send, own_recv)

    def cross_copy(par, c):
        return remote(par, c, OWN, CROSS, cross, cross_send, cross_recv)

    def relay_copy(par, c):
        return remote(par, c, CROSS, RELAYED, partner, relay_send, relay_recv)

    def forward(par, c, first):
        change = dwv[...]
        for t in tiles_of(c):
            rows = pl.ds(t * TILE, TILE)
            if first:
                x_t = xv[rows, :].T
                xt[t] = x_t
            else:
                x_t = xt[t]
            product = jnp.dot(change, x_t, preferred_element_type=jnp.float32)
            ubuf[par, OWN, :, rows] = product.astype(jnp.bfloat16)

    def update_weights(gradient):
        eta = jnp.broadcast_to(eta_ref[...], gradient.shape)
        threshold = eta * lasso_weight
        weights = wv[...]
        stepped = weights + eta * (gradient * (1.0 / samples))
        shrunk = jnp.where(stepped > threshold, stepped - threshold, jnp.where(stepped < -threshold, stepped + threshold, 0.0))
        change = shrunk - weights
        wv[...] = weights + COMBINE_WEIGHT * change
        dwv[...] = change.astype(jnp.bfloat16)

    def wait_sends(par):
        for c in range(count):
            own_copy(par, c).wait_send()
            cross_copy(par, c).wait_send()
            relay_copy(par, c).wait_send()

    def phase(par, first=False, last=False):
        for c in range(count):
            if first:
                x_copy(c).wait()
            forward(par, c, first)
            if c == count // 2 and not first:
                wait_sends(1 - par)
            cross_copy(par, c).start()
            own_copy(par, c).start()
        if first:
            pltpu.make_async_copy(y_hbm, rv, y_sem).wait()
        gradient = None
        for step in range(count + LAG):
            if step < count:
                cross_copy(par, step).wait_recv()
                relay_copy(par, step).start()
            c = step - LAG
            if c < 0:
                continue
            own_copy(par, c).wait_recv()
            relay_copy(par, c).wait_recv()
            rows = rows_of(c)
            u = [ubuf[par, slot, :, rows].astype(jnp.float32) for slot in range(4)]
            total = (u[OWN] + u[PARTNER]) + (u[CROSS] + u[RELAYED])
            residual = rv[:, rows] - (total if first else COMBINE_WEIGHT * total)
            rv[:, rows] = residual
            if not last:
                part = jnp.dot(residual.astype(jnp.bfloat16), xv[rows, :], preferred_element_type=jnp.float32)
                gradient = part if gradient is None else gradient + part
        if not last:
            update_weights(gradient)

    for c in range(count):
        x_copy(c).start()
        if c == 0:
            pltpu.make_async_copy(y_hbm, rv, y_sem).start()
    barrier = pltpu.get_barrier_semaphore()
    for peer in (partner, cross):
        pl.semaphore_signal(barrier, inc=1, device_id={'feat': peer}, device_id_type=MESH)
    wv[...] = w0_ref[...]
    dwv[...] = w0_ref[...].astype(jnp.bfloat16)
    pl.semaphore_wait(barrier, 2)

    phase(0, first=True)

    def sweep(s, carry):
        phase(lax.rem(s, 2))
        return carry

    lax.fori_loop(1, SWEEPS, sweep, 0)
    phase(SWEEPS % 2, last=True)
    wait_sends(SWEEPS % 2)


def solution(mesh):
    group_size = mesh.shape['feat']

    def local_run(x_local, coef_local, targets_local, step_local):
        samples, local_features = x_local.shape
        targets = coef_local.shape[1]
        features = local_features * group_size
        lasso_weight = 0.3 * group_size / features ** 0.5
        chunks = chunk_list(samples)
        count = len(chunks)
        any_spec = pl.BlockSpec(memory_space=pl.ANY)
        vmem_spec = pl.BlockSpec(memory_space=pltpu.VMEM)
        dma = pltpu.SemaphoreType.DMA
        w_t, r_t = pl.pallas_call(
            functools.partial(kernel, chunks, lasso_weight, samples),
            out_shape=(pltpu.VMEM((targets, local_features), jnp.float32), pltpu.VMEM((targets, samples), jnp.float32)),
            in_specs=[pl.BlockSpec(memory_space=pltpu.HBM), vmem_spec, pl.BlockSpec(memory_space=pltpu.HBM), vmem_spec],
            out_specs=(vmem_spec, vmem_spec),
            scratch_shapes=[
                pltpu.VMEM((samples, local_features), jnp.bfloat16),
                pltpu.VMEM((samples // TILE, local_features, TILE), jnp.bfloat16),
                pltpu.VMEM((2, 4, targets, samples), jnp.bfloat16),
                pltpu.VMEM((targets, local_features), jnp.bfloat16),
                dma((count,)), dma,
                dma((2, count)), dma((2, count)), dma((2, count)), dma((2, count)), dma((2, count)), dma((2, count)),
            ],
            compiler_params=pltpu.CompilerParams(collective_id=0, has_side_effects=True, vmem_limit_bytes=60 * 1024 * 1024),
            name='block_lasso',
        )(x_local, coef_local.T, targets_local.T, step_local[None, :])
        return w_t.T, r_t.T

    return jax.shard_map(local_run, mesh=mesh, in_specs=(P('prob', 'feat'), P(('prob', 'feat'), None), P('prob', None), P(('prob', 'feat'))), out_specs=(P(('prob', 'feat'), None), P('prob', None)), check_vma=False)
```

```python
import functools

import jax
import jax.numpy as jnp
from jax import lax
from jax.experimental import pallas as pl
from jax.experimental.pallas import tpu as pltpu
from jax.sharding import PartitionSpec as P

SWEEPS = 6
COMBINE_WEIGHT = 0.8
TILE = 256
MESH = pl.DeviceIdType.MESH
OWN, PARTNER, CROSS, DIAGONAL = 0, 1, 2, 3
PIECE = 512
GROUPS = 6
CHUNK = 1024
TWICE = 0


def kernel(samples, lasso_weight, *refs):
    (x_hbm, w0_ref, y_hbm, eta_ref, wv, rv, xv, xt, ubuf, rbuf, dwv, x_sem, y_sem,
     u_own_send, u_cross_send, u_diag_send, u_own_recv, u_cross_recv, u_diag_recv,
     r_own_send, r_cross_send, r_diag_send, r_own_recv, r_cross_recv, r_diag_recv) = refs
    me = lax.axis_index('feat')
    partner = me + 1 - 2 * lax.rem(me, 2)
    cross = 3 - me
    diagonal = lax.rem(me + 2, 4)
    owned_rows = GROUPS * 4 * PIECE
    units = GROUPS + (samples - owned_rows) // CHUNK
    groups = range(GROUPS)
    shared = range(GROUPS, units)

    def start_of(g, who):
        return g * 4 * PIECE + who * PIECE

    def piece(g, who):
        return pl.ds(pl.multiple_of(start_of(g, who), PIECE), PIECE)

    def chunk(d):
        return pl.ds(owned_rows + (d - GROUPS) * CHUNK, CHUNK)

    def x_copy(unit, who):
        rows = chunk(unit) if who is None else piece(unit, who)
        index = 0 if who is None else who
        return pltpu.make_async_copy(x_hbm.at[rows], xv.at[rows], x_sem.at[unit, index])

    def u_copy(par, unit, rows, src, dst, peer, sems):
        send_sem, recv_sem = sems
        return pltpu.make_async_remote_copy(
            src_ref=ubuf.at[par, src, :, rows], dst_ref=ubuf.at[par, dst, :, rows],
            send_sem=send_sem.at[par, unit], recv_sem=recv_sem.at[par, unit], device_id={'feat': peer}, device_id_type=MESH)

    def r_copy(par, last, g, who, peer, sems):
        send_sem, recv_sem = sems
        rows = piece(g, who)
        ref = rv.at[:, rows] if last else rbuf.at[par, :, rows]
        return pltpu.make_async_remote_copy(
            src_ref=ref, dst_ref=ref, send_sem=send_sem.at[par, g], recv_sem=recv_sem.at[par, g], device_id={'feat': peer}, device_id_type=MESH)

    own_sems, cross_sems, diag_sems = (u_own_send, u_own_recv), (u_cross_send, u_cross_recv), (u_diag_send, u_diag_recv)
    r_own_sems, r_cross_sems, r_diag_sems = (r_own_send, r_own_recv), (r_cross_send, r_cross_recv), (r_diag_send, r_diag_recv)

    def group_copies(par, g, receive=False):
        rows = [piece(g, me)] * 3 if receive else [piece(g, cross), piece(g, diagonal), piece(g, partner)]
        return [u_copy(par, g, rows[0], OWN, CROSS, cross, cross_sems), u_copy(par, g, rows[1], OWN, DIAGONAL, diagonal, diag_sems), u_copy(par, g, rows[2], OWN, PARTNER, partner, own_sems)]

    def chunk_copies(par, d):
        rows = chunk(d)
        return [u_copy(par, d, rows, OWN, CROSS, cross, cross_sems), u_copy(par, d, rows, OWN, PARTNER, partner, own_sems), u_copy(par, d, rows, CROSS, DIAGONAL, partner, diag_sems)]

    def r_twice(g):
        return g >= GROUPS - TWICE

    def return_copies(par, last, g):
        return [r_copy(par, last, g, me, cross, r_cross_sems), r_copy(par, last, g, me, partner, r_own_sems),
                r_copy(par, last, g, me, diagonal, r_diag_sems) if r_twice(g) else r_copy(par, last, g, cross, partner, r_diag_sems)]

    def forward(par, start, size, first):
        change = dwv[...]
        for i in range(size // TILE):
            rows = pl.ds(start + i * TILE if isinstance(start, int) else pl.multiple_of(start + i * TILE, TILE), TILE)
            t = start // TILE + i
            if first:
                x_t = xv[rows, :].T
                xt[t] = x_t
            else:
                x_t = xt[t]
            product = jnp.dot(change, x_t, preferred_element_type=jnp.float32)
            ubuf[par, OWN, :, rows] = product.astype(jnp.bfloat16)

    def new_residual(par, rows, first):
        u = [ubuf[par, slot, :, rows].astype(jnp.float32) for slot in range(4)]
        total = (u[OWN] + u[PARTNER]) + (u[CROSS] + u[DIAGONAL])
        residual = rv[:, rows] - (total if first else COMBINE_WEIGHT * total)
        rv[:, rows] = residual
        return residual

    def update_weights(gradient):
        eta = jnp.broadcast_to(eta_ref[...], gradient.shape)
        threshold = eta * lasso_weight
        weights = wv[...]
        stepped = weights + eta * (gradient * (1.0 / samples))
        shrunk = jnp.where(stepped > threshold, stepped - threshold, jnp.where(stepped < -threshold, stepped + threshold, 0.0))
        change = shrunk - weights
        wv[...] = weights + COMBINE_WEIGHT * change
        dwv[...] = change.astype(jnp.bfloat16)

    def wait_sends(par, last=False):
        for g in groups:
            for copy in group_copies(par, g) + return_copies(par, last, g):
                copy.wait_send()
        for d in shared:
            for copy in chunk_copies(par, d):
                copy.wait_send()

    def phase(par, first=False, last=False):
        parts = []

        def add_gradient(lhs, rows):
            part = jnp.dot(lhs, xv[rows, :], preferred_element_type=jnp.float32)
            parts[:] = [part if not parts else parts[0] + part]

        for g in groups:
            for i, who in enumerate((cross, diagonal, partner, me)):
                if first:
                    x_copy(g, who).wait()
                forward(par, start_of(g, who), PIECE, first)
                if i < 3:
                    group_copies(par, g)[i].start()
        for d in shared:
            if first:
                x_copy(d, None).wait()
            forward(par, owned_rows + (d - GROUPS) * CHUNK, CHUNK, first)
            if d == units - 1 and not first:
                wait_sends(1 - par)
            to_cross, to_partner, _ = chunk_copies(par, d)
            to_cross.start()
            to_partner.start()
        if first:
            pltpu.make_async_copy(y_hbm, rv, y_sem).wait()

        def owner_step(g):
            for copy in group_copies(par, g, receive=True):
                copy.wait_recv()
            rows = piece(g, me)
            residual = new_residual(par, rows, first)
            if not last:
                rounded = residual.astype(jnp.bfloat16)
                rbuf[par, :, rows] = rounded
            to_cross, to_partner, third = return_copies(par, last, g)
            to_cross.start()
            if r_twice(g):
                third.start()
            to_partner.start()
            if not last:
                add_gradient(rounded, rows)

        def take(g, who):
            if not last:
                add_gradient(rbuf[par, :, piece(g, who)], piece(g, who))

        def partner_step(g):
            r_copy(par, last, g, partner, partner, r_own_sems).wait_recv()
            take(g, partner)

        def cross_step(g):
            r_copy(par, last, g, cross, cross, r_cross_sems).wait_recv()
            if not r_twice(g):
                return_copies(par, last, g)[2].start()
            take(g, cross)

        def diagonal_step(g):
            r_copy(par, last, g, diagonal, partner, r_diag_sems).wait_recv()
            take(g, diagonal)

        def relay_step(d):
            to_cross, _, relay = chunk_copies(par, d)
            to_cross.wait_recv()
            relay.start()

        def shared_step(d):
            _, to_partner, relay = chunk_copies(par, d)
            to_partner.wait_recv()
            relay.wait_recv()
            residual = new_residual(par, chunk(d), first)
            if not last:
                add_gradient(residual.astype(jnp.bfloat16), chunk(d))

        for g in groups:
            owner_step(g)
        for d in shared:
            relay_step(d)
        for g in groups:
            partner_step(g)
        waiting = list(shared)
        for g in groups:
            if waiting and g % 2 == 0:
                shared_step(waiting.pop(0))
            cross_step(g)
        for d in waiting:
            shared_step(d)
        for g in groups:
            diagonal_step(g)
        if not last:
            update_weights(parts[0])

    for g in groups:
        for who in (cross, diagonal, partner, me):
            x_copy(g, who).start()
        if g == 0:
            pltpu.make_async_copy(y_hbm, rv, y_sem).start()
    for d in shared:
        x_copy(d, None).start()
    barrier = pltpu.get_barrier_semaphore()
    for peer in (partner, cross, diagonal):
        pl.semaphore_signal(barrier, inc=1, device_id={'feat': peer}, device_id_type=MESH)
    wv[...] = w0_ref[...]
    dwv[...] = w0_ref[...].astype(jnp.bfloat16)
    pl.semaphore_wait(barrier, 3)

    phase(0, first=True)

    def sweep(s, carry):
        phase(lax.rem(s, 2))
        return carry

    lax.fori_loop(1, SWEEPS, sweep, 0)
    phase(SWEEPS % 2, last=True)
    wait_sends(SWEEPS % 2, last=True)


def solution(mesh):
    group_size = mesh.shape['feat']

    def local_run(x_local, coef_local, targets_local, step_local):
        samples, local_features = x_local.shape
        targets = coef_local.shape[1]
        features = local_features * group_size
        lasso_weight = 0.3 * group_size / features ** 0.5
        units = GROUPS + (samples - GROUPS * 4 * PIECE) // CHUNK
        hbm_spec = pl.BlockSpec(memory_space=pltpu.HBM)
        vmem_spec = pl.BlockSpec(memory_space=pltpu.VMEM)
        dma = pltpu.SemaphoreType.DMA
        w_t, r_t = pl.pallas_call(
            functools.partial(kernel, samples, lasso_weight),
            out_shape=(pltpu.VMEM((targets, local_features), jnp.float32), pltpu.VMEM((targets, samples), jnp.float32)),
            in_specs=[hbm_spec, vmem_spec, hbm_spec, vmem_spec],
            out_specs=(vmem_spec, vmem_spec),
            scratch_shapes=[
                pltpu.VMEM((samples, local_features), jnp.bfloat16),
                pltpu.VMEM((samples // TILE, local_features, TILE), jnp.bfloat16),
                pltpu.VMEM((2, 4, targets, samples), jnp.bfloat16),
                pltpu.VMEM((2, targets, samples), jnp.bfloat16),
                pltpu.VMEM((targets, local_features), jnp.bfloat16),
                dma((units, 4)), dma,
                *[dma((2, units))] * 6, *[dma((2, GROUPS))] * 6,
            ],
            compiler_params=pltpu.CompilerParams(collective_id=0, has_side_effects=True, vmem_limit_bytes=60 * 1024 * 1024),
            name='block_lasso',
        )(x_local, coef_local.T, targets_local.T, step_local[None, :])
        return w_t.T, r_t.T

    return jax.shard_map(local_run, mesh=mesh, in_specs=(P('prob', 'feat'), P(('prob', 'feat'), None), P('prob', None), P(('prob', 'feat'))), out_specs=(P(('prob', 'feat'), None), P('prob', None)), check_vma=False)
```

```python
import functools

import jax
import jax.numpy as jnp
from jax import lax
from jax.experimental import pallas as pl
from jax.experimental.pallas import tpu as pltpu
from jax.sharding import PartitionSpec as P

SWEEPS = 6
COMBINE_WEIGHT = 0.8
LAG = 3
TWICE = 1
TILE = 256
MESH = pl.DeviceIdType.MESH
OWN, PARTNER, CROSS, RELAYED = 0, 1, 2, 3


def chunk_list(samples):
    sizes = [512, 512] + [1024] * ((samples - 2048) // 1024) + [512, 512]
    return [(sum(sizes[:i]), size) for i, size in enumerate(sizes)]


def kernel(chunks, lasso_weight, samples, *refs):
    (x_hbm, w0_ref, y_hbm, eta_ref, wv, rv, xv, xt, ubuf, dwv, x_sem, y_sem,
     own_send, cross_send, relay_send, own_recv, cross_recv, relay_recv) = refs
    count = len(chunks)
    targets = w0_ref.shape[0]
    me = lax.axis_index('feat')
    partner = me + 1 - 2 * lax.rem(me, 2)
    cross = 3 - me
    diagonal = lax.rem(me + 2, 4)

    def rows_of(c):
        start, size = chunks[c]
        return pl.ds(start, size)

    def tiles_of(c):
        start, size = chunks[c]
        return range(start // TILE, (start + size) // TILE)

    def x_copy(c):
        return pltpu.make_async_copy(x_hbm.at[rows_of(c)], xv.at[rows_of(c)], x_sem.at[c])

    def remote(par, c, src, dst, peer, send_sem, recv_sem):
        return pltpu.make_async_remote_copy(
            src_ref=ubuf.at[par, src, :, rows_of(c)], dst_ref=ubuf.at[par, dst, :, rows_of(c)],
            send_sem=send_sem.at[par, c], recv_sem=recv_sem.at[par, c], device_id={'feat': peer}, device_id_type=MESH)

    def own_copy(par, c):
        return remote(par, c, OWN, PARTNER, partner, own_send, own_recv)

    def cross_copy(par, c):
        return remote(par, c, OWN, CROSS, cross, cross_send, cross_recv)

    def twice(c):
        return c >= count - TWICE

    def relay_copy(par, c):
        if twice(c):
            return remote(par, c, OWN, RELAYED, diagonal, relay_send, relay_recv)
        return remote(par, c, CROSS, RELAYED, partner, relay_send, relay_recv)

    def forward(par, c, first):
        change = dwv[...]
        for t in tiles_of(c):
            rows = pl.ds(t * TILE, TILE)
            if first:
                x_t = xv[rows, :].T
                xt[t] = x_t
            else:
                x_t = xt[t]
            product = jnp.dot(change, x_t, preferred_element_type=jnp.float32)
            ubuf[par, OWN, :, rows] = product.astype(jnp.bfloat16)

    def update_weights(gradient):
        eta = jnp.broadcast_to(eta_ref[...], gradient.shape)
        threshold = eta * lasso_weight
        weights = wv[...]
        stepped = weights + eta * (gradient * (1.0 / samples))
        shrunk = jnp.where(stepped > threshold, stepped - threshold, jnp.where(stepped < -threshold, stepped + threshold, 0.0))
        change = shrunk - weights
        wv[...] = weights + COMBINE_WEIGHT * change
        dwv[...] = change.astype(jnp.bfloat16)

    def wait_sends(par):
        for c in range(count):
            own_copy(par, c).wait_send()
            cross_copy(par, c).wait_send()
            relay_copy(par, c).wait_send()

    def phase(par, first=False, last=False):
        for c in range(count):
            if first:
                x_copy(c).wait()
            forward(par, c, first)
            if c == count // 2 and not first:
                wait_sends(1 - par)
            if twice(c):
                relay_copy(par, c).start()
            cross_copy(par, c).start()
            own_copy(par, c).start()
        if first:
            pltpu.make_async_copy(y_hbm, rv, y_sem).wait()
        gradient = None
        for step in range(count + LAG):
            if step < count:
                cross_copy(par, step).wait_recv()
                if not twice(step):
                    relay_copy(par, step).start()
            c = step - LAG
            if c < 0:
                continue
            own_copy(par, c).wait_recv()
            relay_copy(par, c).wait_recv()
            rows = rows_of(c)
            u = [ubuf[par, slot, :, rows].astype(jnp.float32) for slot in range(4)]
            total = (u[OWN] + u[PARTNER]) + (u[CROSS] + u[RELAYED])
            residual = rv[:, rows] - (total if first else COMBINE_WEIGHT * total)
            rv[:, rows] = residual
            if not last:
                part = jnp.dot(residual.astype(jnp.bfloat16), xv[rows, :], preferred_element_type=jnp.float32)
                gradient = part if gradient is None else gradient + part
        if not last:
            update_weights(gradient)

    for c in range(count):
        x_copy(c).start()
        if c == 0:
            pltpu.make_async_copy(y_hbm, rv, y_sem).start()
    barrier = pltpu.get_barrier_semaphore()
    for peer in (partner, cross, diagonal):
        pl.semaphore_signal(barrier, inc=1, device_id={'feat': peer}, device_id_type=MESH)
    wv[...] = w0_ref[...]
    dwv[...] = w0_ref[...].astype(jnp.bfloat16)
    pl.semaphore_wait(barrier, 3)

    phase(0, first=True)

    def sweep(s, carry):
        phase(lax.rem(s, 2))
        return carry

    lax.fori_loop(1, SWEEPS, sweep, 0)
    phase(SWEEPS % 2, last=True)
    wait_sends(SWEEPS % 2)


def solution(mesh):
    group_size = mesh.shape['feat']

    def local_run(x_local, coef_local, targets_local, step_local):
        samples, local_features = x_local.shape
        targets = coef_local.shape[1]
        features = local_features * group_size
        lasso_weight = 0.3 * group_size / features ** 0.5
        chunks = chunk_list(samples)
        count = len(chunks)
        any_spec = pl.BlockSpec(memory_space=pl.ANY)
        vmem_spec = pl.BlockSpec(memory_space=pltpu.VMEM)
        dma = pltpu.SemaphoreType.DMA
        w_t, r_t = pl.pallas_call(
            functools.partial(kernel, chunks, lasso_weight, samples),
            out_shape=(pltpu.VMEM((targets, local_features), jnp.float32), pltpu.VMEM((targets, samples), jnp.float32)),
            in_specs=[pl.BlockSpec(memory_space=pltpu.HBM), vmem_spec, pl.BlockSpec(memory_space=pltpu.HBM), vmem_spec],
            out_specs=(vmem_spec, vmem_spec),
            scratch_shapes=[
                pltpu.VMEM((samples, local_features), jnp.bfloat16),
                pltpu.VMEM((samples // TILE, local_features, TILE), jnp.bfloat16),
                pltpu.VMEM((2, 4, targets, samples), jnp.bfloat16),
                pltpu.VMEM((targets, local_features), jnp.bfloat16),
                dma((count,)), dma,
                dma((2, count)), dma((2, count)), dma((2, count)), dma((2, count)), dma((2, count)), dma((2, count)),
            ],
            compiler_params=pltpu.CompilerParams(collective_id=0, has_side_effects=True, vmem_limit_bytes=60 * 1024 * 1024),
            name='block_lasso',
        )(x_local, coef_local.T, targets_local.T, step_local[None, :])
        return w_t.T, r_t.T

    return jax.shard_map(local_run, mesh=mesh, in_specs=(P('prob', 'feat'), P(('prob', 'feat'), None), P('prob', None), P(('prob', 'feat'))), out_specs=(P(('prob', 'feat'), None), P('prob', None)), check_vma=False)
```

```python
import functools

import jax
import jax.numpy as jnp
from jax import lax
from jax.experimental import pallas as pl
from jax.experimental.pallas import tpu as pltpu
from jax.sharding import PartitionSpec as P

SWEEPS = 6
COMBINE_WEIGHT = 0.8
LAG = 2
TILE = 256
MESH = pl.DeviceIdType.MESH
OWN, PARTNER, CROSS, RELAYED = 0, 1, 2, 3


def chunk_list(samples):
    size = samples // 8
    return [(i * size, size) for i in range(8)]


def kernel(chunks, lasso_weight, samples, *refs):
    (x_hbm, w0_ref, y_hbm, eta_ref, wv, rv, xv, xt, ubuf, dwv, x_sem, y_sem,
     own_send, cross_send, relay_send, own_recv, cross_recv, relay_recv) = refs
    count = len(chunks)
    targets = w0_ref.shape[0]
    me = lax.axis_index('feat')
    partner = me + 1 - 2 * lax.rem(me, 2)
    cross = 3 - me

    def rows_of(c):
        start, size = chunks[c]
        return pl.ds(start, size)

    def tiles_of(c):
        start, size = chunks[c]
        return range(start // TILE, (start + size) // TILE)

    def x_copy(c):
        return pltpu.make_async_copy(x_hbm.at[rows_of(c)], xv.at[rows_of(c)], x_sem.at[c])

    def remote(par, c, src, dst, peer, send_sem, recv_sem):
        return pltpu.make_async_remote_copy(
            src_ref=ubuf.at[par, src, :, rows_of(c)], dst_ref=ubuf.at[par, dst, :, rows_of(c)],
            send_sem=send_sem.at[par, c], recv_sem=recv_sem.at[par, c], device_id={'feat': peer}, device_id_type=MESH)

    def own_copy(par, c):
        return remote(par, c, OWN, PARTNER, partner, own_send, own_recv)

    def cross_copy(par, c):
        return remote(par, c, OWN, CROSS, cross, cross_send, cross_recv)

    def relay_copy(par, c):
        return remote(par, c, CROSS, RELAYED, partner, relay_send, relay_recv)

    def forward(par, c, first):
        change = dwv[...]
        for t in tiles_of(c):
            rows = pl.ds(t * TILE, TILE)
            if first:
                x_t = xv[rows, :].T
                xt[t] = x_t
            else:
                x_t = xt[t]
            product = jnp.dot(change, x_t, preferred_element_type=jnp.float32)
            ubuf[par, OWN, :, rows] = product.astype(jnp.bfloat16)

    def update_weights(gradient):
        eta = jnp.broadcast_to(eta_ref[...], gradient.shape)
        threshold = eta * lasso_weight
        weights = wv[...]
        stepped = weights + eta * (gradient * (1.0 / samples))
        shrunk = jnp.where(stepped > threshold, stepped - threshold, jnp.where(stepped < -threshold, stepped + threshold, 0.0))
        change = shrunk - weights
        wv[...] = weights + COMBINE_WEIGHT * change
        dwv[...] = change.astype(jnp.bfloat16)

    def wait_sends(par):
        for c in range(count):
            own_copy(par, c).wait_send()
            cross_copy(par, c).wait_send()
            relay_copy(par, c).wait_send()

    def phase(par, first=False, last=False):
        for c in range(count):
            if first:
                x_copy(c).wait()
            forward(par, c, first)
            if c == count // 2 and not first:
                wait_sends(1 - par)
            cross_copy(par, c).start()
            own_copy(par, c).start()
        if first:
            pltpu.make_async_copy(y_hbm, rv, y_sem).wait()
        gradient = None
        for step in range(count + LAG):
            if step < count:
                cross_copy(par, step).wait_recv()
                relay_copy(par, step).start()
            c = step - LAG
            if c < 0:
                continue
            own_copy(par, c).wait_recv()
            relay_copy(par, c).wait_recv()
            rows = rows_of(c)
            u = [ubuf[par, slot, :, rows].astype(jnp.float32) for slot in range(4)]
            total = (u[OWN] + u[PARTNER]) + (u[CROSS] + u[RELAYED])
            residual = rv[:, rows] - (total if first else COMBINE_WEIGHT * total)
            rv[:, rows] = residual
            if not last:
                part = jnp.dot(residual.astype(jnp.bfloat16), xv[rows, :], preferred_element_type=jnp.float32)
                gradient = part if gradient is None else gradient + part
        if not last:
            update_weights(gradient)

    for c in range(count):
        x_copy(c).start()
        if c == 0:
            pltpu.make_async_copy(y_hbm, rv, y_sem).start()
    barrier = pltpu.get_barrier_semaphore()
    for peer in (partner, cross):
        pl.semaphore_signal(barrier, inc=1, device_id={'feat': peer}, device_id_type=MESH)
    wv[...] = w0_ref[...]
    dwv[...] = w0_ref[...].astype(jnp.bfloat16)
    pl.semaphore_wait(barrier, 2)

    phase(0, first=True)

    def sweep(s, carry):
        phase(lax.rem(s, 2))
        return carry

    lax.fori_loop(1, SWEEPS, sweep, 0)
    phase(SWEEPS % 2, last=True)
    wait_sends(SWEEPS % 2)


def solution(mesh):
    group_size = mesh.shape['feat']

    def local_run(x_local, coef_local, targets_local, step_local):
        samples, local_features = x_local.shape
        targets = coef_local.shape[1]
        features = local_features * group_size
        lasso_weight = 0.3 * group_size / features ** 0.5
        chunks = chunk_list(samples)
        count = len(chunks)
        any_spec = pl.BlockSpec(memory_space=pl.ANY)
        vmem_spec = pl.BlockSpec(memory_space=pltpu.VMEM)
        dma = pltpu.SemaphoreType.DMA
        w_t, r_t = pl.pallas_call(
            functools.partial(kernel, chunks, lasso_weight, samples),
            out_shape=(pltpu.VMEM((targets, local_features), jnp.float32), pltpu.VMEM((targets, samples), jnp.float32)),
            in_specs=[pl.BlockSpec(memory_space=pltpu.HBM), vmem_spec, pl.BlockSpec(memory_space=pltpu.HBM), vmem_spec],
            out_specs=(vmem_spec, vmem_spec),
            scratch_shapes=[
                pltpu.VMEM((samples, local_features), jnp.bfloat16),
                pltpu.VMEM((samples // TILE, local_features, TILE), jnp.bfloat16),
                pltpu.VMEM((2, 4, targets, samples), jnp.bfloat16),
                pltpu.VMEM((targets, local_features), jnp.bfloat16),
                dma((count,)), dma,
                dma((2, count)), dma((2, count)), dma((2, count)), dma((2, count)), dma((2, count)), dma((2, count)),
            ],
            compiler_params=pltpu.CompilerParams(collective_id=0, has_side_effects=True, vmem_limit_bytes=60 * 1024 * 1024),
            name='block_lasso',
        )(x_local, coef_local.T, targets_local.T, step_local[None, :])
        return w_t.T, r_t.T

    return jax.shard_map(local_run, mesh=mesh, in_specs=(P('prob', 'feat'), P(('prob', 'feat'), None), P('prob', None), P(('prob', 'feat'))), out_specs=(P(('prob', 'feat'), None), P('prob', None)), check_vma=False)
```

```python
import functools

import jax
import jax.numpy as jnp
from jax import lax
from jax.experimental import pallas as pl
from jax.experimental.pallas import tpu as pltpu
from jax.sharding import PartitionSpec as P

SWEEPS = 6
COMBINE_WEIGHT = 0.8
LAG = 2
TILE = 256
MESH = pl.DeviceIdType.MESH
OWN, PARTNER, CROSS, RELAYED = 0, 1, 2, 3


def chunk_list(samples):
    sizes = [512, 1536] + [2048] * (samples // 2048 - 2) + [1024, 1024]
    return [(sum(sizes[:i]), size) for i, size in enumerate(sizes)]


def kernel(chunks, lasso_weight, samples, *refs):
    (x_hbm, w0_ref, y_hbm, eta_ref, wv, rv, xv, xt, ubuf, rbuf, dwv, x_sem, y_sem,
     own_send, cross_send, relay_send, own_recv, cross_recv, relay_recv) = refs
    count = len(chunks)
    targets = w0_ref.shape[0]
    me = lax.axis_index('feat')
    partner = me + 1 - 2 * lax.rem(me, 2)
    cross = 3 - me

    def rows_of(c):
        if c is None:
            return pl.ds(0, samples)
        start, size = chunks[c]
        return pl.ds(start, size)

    def tiles_of(c):
        start, size = chunks[c]
        return range(start // TILE, (start + size) // TILE)

    def x_copy(c):
        return pltpu.make_async_copy(x_hbm.at[rows_of(c)], xv.at[rows_of(c)], x_sem.at[c])

    def remote(par, c, src, dst, peer, send_sem, recv_sem):
        return pltpu.make_async_remote_copy(
            src_ref=ubuf.at[par, src, :, rows_of(c)], dst_ref=ubuf.at[par, dst, :, rows_of(c)],
            send_sem=send_sem.at[par], recv_sem=recv_sem.at[par] if c is None or src == dst - 1 == OWN else recv_sem.at[par, c], device_id={'feat': peer}, device_id_type=MESH)

    def own_copy(par, c):
        return remote(par, c, OWN, PARTNER, partner, own_send, own_recv)

    def cross_copy(par, c):
        return remote(par, c, OWN, CROSS, cross, cross_send, cross_recv)

    def relay_copy(par, c):
        return remote(par, c, CROSS, RELAYED, partner, relay_send, relay_recv)

    def forward(par, c, first):
        change = dwv[...]
        for t in tiles_of(c):
            rows = pl.ds(t * TILE, TILE)
            if first:
                x_t = xv[rows, :].T
                xt[t] = x_t
            else:
                x_t = xt[t]
            product = jnp.dot(change, x_t, preferred_element_type=jnp.float32)
            ubuf[par, OWN, :, rows] = product.astype(jnp.bfloat16)

    def update_weights(gradient):
        eta = jnp.broadcast_to(eta_ref[...], gradient.shape)
        threshold = eta * lasso_weight
        weights = wv[...]
        stepped = weights + eta * (gradient * (1.0 / samples))
        shrunk = jnp.where(stepped > threshold, stepped - threshold, jnp.where(stepped < -threshold, stepped + threshold, 0.0))
        change = shrunk - weights
        wv[...] = weights + COMBINE_WEIGHT * change
        dwv[...] = change.astype(jnp.bfloat16)

    def wait_sends(par):
        own_copy(par, None).wait_send()
        cross_copy(par, None).wait_send()
        relay_copy(par, None).wait_send()

    def phase(par, first=False, last=False):
        for c in range(count):
            if first:
                x_copy(c).wait()
            forward(par, c, first)
            if c == count // 2 and not first:
                wait_sends(1 - par)
            cross_copy(par, c).start()
            own_copy(par, c).start()
        if first:
            pltpu.make_async_copy(y_hbm, rv, y_sem).wait()
        gradient = None
        for step in range(count + LAG + 1):
            if step < count:
                cross_copy(par, step).wait_recv()
                relay_copy(par, step).start()
            c = step - LAG
            if c == 0:
                own_copy(par, None).wait_recv()
            if 0 <= c < count:
                relay_copy(par, c).wait_recv()
                rows = rows_of(c)
                u = [ubuf[par, slot, :, rows].astype(jnp.float32) for slot in range(4)]
                total = (u[OWN] + u[PARTNER]) + (u[CROSS] + u[RELAYED])
                residual = rv[:, rows] - (total if first else COMBINE_WEIGHT * total)
                rv[:, rows] = residual
                rbuf[:, rows] = residual.astype(jnp.bfloat16)
            if c >= 1 and not last:
                rows = rows_of(c - 1)
                part = jnp.dot(rbuf[:, rows], xv[rows, :], preferred_element_type=jnp.float32)
                gradient = part if gradient is None else gradient + part
        if not last:
            update_weights(gradient)

    for c in range(count):
        x_copy(c).start()
        if c == 0:
            pltpu.make_async_copy(y_hbm, rv, y_sem).start()
    barrier = pltpu.get_barrier_semaphore()
    for peer in (partner, cross):
        pl.semaphore_signal(barrier, inc=1, device_id={'feat': peer}, device_id_type=MESH)
    wv[...] = w0_ref[...]
    dwv[...] = w0_ref[...].astype(jnp.bfloat16)
    pl.semaphore_wait(barrier, 2)

    phase(0, first=True)

    def sweep(s, carry):
        phase(lax.rem(s, 2))
        return carry

    lax.fori_loop(1, SWEEPS, sweep, 0)
    phase(SWEEPS % 2, last=True)
    wait_sends(SWEEPS % 2)


def solution(mesh):
    group_size = mesh.shape['feat']

    def local_run(x_local, coef_local, targets_local, step_local):
        samples, local_features = x_local.shape
        targets = coef_local.shape[1]
        features = local_features * group_size
        lasso_weight = 0.3 * group_size / features ** 0.5
        chunks = chunk_list(samples)
        count = len(chunks)
        any_spec = pl.BlockSpec(memory_space=pl.ANY)
        vmem_spec = pl.BlockSpec(memory_space=pltpu.VMEM)
        dma = pltpu.SemaphoreType.DMA
        w_t, r_t = pl.pallas_call(
            functools.partial(kernel, chunks, lasso_weight, samples),
            out_shape=(pltpu.VMEM((targets, local_features), jnp.float32), pltpu.VMEM((targets, samples), jnp.float32)),
            in_specs=[pl.BlockSpec(memory_space=pltpu.HBM), vmem_spec, pl.BlockSpec(memory_space=pltpu.HBM), vmem_spec],
            out_specs=(vmem_spec, vmem_spec),
            scratch_shapes=[
                pltpu.VMEM((samples, local_features), jnp.bfloat16),
                pltpu.VMEM((samples // TILE, local_features, TILE), jnp.bfloat16),
                pltpu.VMEM((2, 4, targets, samples), jnp.bfloat16),
                pltpu.VMEM((targets, samples), jnp.bfloat16),
                pltpu.VMEM((targets, local_features), jnp.bfloat16),
                dma((count,)), dma,
                dma((2,)), dma((2,)), dma((2,)), dma((2,)), dma((2, count)), dma((2, count)),
            ],
            compiler_params=pltpu.CompilerParams(collective_id=0, has_side_effects=True, vmem_limit_bytes=60 * 1024 * 1024),
            name='block_lasso',
        )(x_local, coef_local.T, targets_local.T, step_local[None, :])
        return w_t.T, r_t.T

    return jax.shard_map(local_run, mesh=mesh, in_specs=(P('prob', 'feat'), P(('prob', 'feat'), None), P('prob', None), P(('prob', 'feat'))), out_specs=(P(('prob', 'feat'), None), P('prob', None)), check_vma=False)
```

```python
import functools

import jax
import jax.numpy as jnp
from jax import lax
from jax.experimental import pallas as pl
from jax.experimental.pallas import tpu as pltpu
from jax.sharding import PartitionSpec as P

SWEEPS = 6
COMBINE_WEIGHT = 0.8
LAG = 2
LATE = (1, 3, 5, 7)
TILE = 256
MESH = pl.DeviceIdType.MESH
OWN, PARTNER, CROSS, RELAYED = 0, 1, 2, 3


def chunk_list(samples):
    sizes = [512, 1536] + [2048] * (samples // 2048 - 2) + [1024, 1024]
    return [(sum(sizes[:i]), size) for i, size in enumerate(sizes)]


def kernel(chunks, lasso_weight, samples, *refs):
    (x_hbm, w0_ref, y_hbm, eta_ref, wv, rv, xv, xt, ubuf, rbuf, dwv, x_sem, y_sem,
     own_send, cross_send, relay_send, own_recv, cross_recv, relay_recv) = refs
    count = len(chunks)
    targets = w0_ref.shape[0]
    me = lax.axis_index('feat')
    partner = me + 1 - 2 * lax.rem(me, 2)
    cross = 3 - me

    def rows_of(c):
        if c is None:
            return pl.ds(0, samples)
        start, size = chunks[c]
        return pl.ds(start, size)

    def tiles_of(c):
        start, size = chunks[c]
        return range(start // TILE, (start + size) // TILE)

    def x_copy(c):
        return pltpu.make_async_copy(x_hbm.at[rows_of(c)], xv.at[rows_of(c)], x_sem.at[c])

    def remote(par, c, src, dst, peer, send_sem, recv_sem):
        return pltpu.make_async_remote_copy(
            src_ref=ubuf.at[par, src, :, rows_of(c)], dst_ref=ubuf.at[par, dst, :, rows_of(c)],
            send_sem=send_sem.at[par], recv_sem=recv_sem.at[par] if c is None or src == dst - 1 == OWN else recv_sem.at[par, c], device_id={'feat': peer}, device_id_type=MESH)

    def own_copy(par, c):
        return remote(par, c, OWN, PARTNER, partner, own_send, own_recv)

    def cross_copy(par, c):
        return remote(par, c, OWN, CROSS, cross, cross_send, cross_recv)

    def relay_copy(par, c):
        return remote(par, c, CROSS, RELAYED, partner, relay_send, relay_recv)

    def transpose_x(c):
        for t in tiles_of(c):
            xt[t] = xv[pl.ds(t * TILE, TILE), :].T

    def forward(par, c, first):
        change = dwv[...]
        for t in tiles_of(c):
            rows = pl.ds(t * TILE, TILE)
            if first:
                product = lax.dot_general(change, xv[rows, :], (((1,), (1,)), ((), ())), preferred_element_type=jnp.float32)
            else:
                product = jnp.dot(change, xt[t], preferred_element_type=jnp.float32)
            ubuf[par, OWN, :, rows] = product.astype(jnp.bfloat16)
        if first and c not in LATE:
            transpose_x(c)

    def update_weights(gradient):
        eta = jnp.broadcast_to(eta_ref[...], gradient.shape)
        threshold = eta * lasso_weight
        weights = wv[...]
        stepped = weights + eta * (gradient * (1.0 / samples))
        shrunk = jnp.where(stepped > threshold, stepped - threshold, jnp.where(stepped < -threshold, stepped + threshold, 0.0))
        change = shrunk - weights
        wv[...] = weights + COMBINE_WEIGHT * change
        dwv[...] = change.astype(jnp.bfloat16)

    def wait_sends(par):
        own_copy(par, None).wait_send()
        cross_copy(par, None).wait_send()
        relay_copy(par, None).wait_send()

    def phase(par, first=False, last=False):
        for c in range(count):
            if first:
                x_copy(c).wait()
            forward(par, c, first)
            if c == count // 2 and not first:
                wait_sends(1 - par)
            if first and c == 0:
                pl.semaphore_wait(barrier, 2)
            cross_copy(par, c).start()
            own_copy(par, c).start()
        if first:
            pltpu.make_async_copy(y_hbm, rv, y_sem).wait()
        gradient = None
        for step in range(count + LAG + 1):
            if step < count:
                cross_copy(par, step).wait_recv()
                relay_copy(par, step).start()
            if first and step in LATE:
                transpose_x(step)
            c = step - LAG
            if c == 0:
                own_copy(par, None).wait_recv()
            if 0 <= c < count:
                relay_copy(par, c).wait_recv()
                rows = rows_of(c)
                u = [ubuf[par, slot, :, rows].astype(jnp.float32) for slot in range(4)]
                total = (u[OWN] + u[PARTNER]) + (u[CROSS] + u[RELAYED])
                residual = rv[:, rows] - (total if first else COMBINE_WEIGHT * total)
                rv[:, rows] = residual
                rbuf[:, rows] = residual.astype(jnp.bfloat16)
            if c >= 1 and not last:
                rows = rows_of(c - 1)
                part = jnp.dot(rbuf[:, rows], xv[rows, :], preferred_element_type=jnp.float32)
                gradient = part if gradient is None else gradient + part
        if not last:
            update_weights(gradient)

    for c in range(count):
        x_copy(c).start()
        if c == 0:
            pltpu.make_async_copy(y_hbm, rv, y_sem).start()
    barrier = pltpu.get_barrier_semaphore()
    for peer in (partner, cross):
        pl.semaphore_signal(barrier, inc=1, device_id={'feat': peer}, device_id_type=MESH)
    wv[...] = w0_ref[...]
    dwv[...] = w0_ref[...].astype(jnp.bfloat16)
    phase(0, first=True)

    def sweep(s, carry):
        phase(lax.rem(s, 2))
        return carry

    lax.fori_loop(1, SWEEPS, sweep, 0)
    phase(SWEEPS % 2, last=True)
    wait_sends(SWEEPS % 2)


def solution(mesh):
    group_size = mesh.shape['feat']

    def local_run(x_local, coef_local, targets_local, step_local):
        samples, local_features = x_local.shape
        targets = coef_local.shape[1]
        features = local_features * group_size
        lasso_weight = 0.3 * group_size / features ** 0.5
        chunks = chunk_list(samples)
        count = len(chunks)
        any_spec = pl.BlockSpec(memory_space=pl.ANY)
        vmem_spec = pl.BlockSpec(memory_space=pltpu.VMEM)
        dma = pltpu.SemaphoreType.DMA
        w_t, r_t = pl.pallas_call(
            functools.partial(kernel, chunks, lasso_weight, samples),
            out_shape=(pltpu.VMEM((targets, local_features), jnp.float32), pltpu.VMEM((targets, samples), jnp.float32)),
            in_specs=[pl.BlockSpec(memory_space=pltpu.HBM), vmem_spec, pl.BlockSpec(memory_space=pltpu.HBM), vmem_spec],
            out_specs=(vmem_spec, vmem_spec),
            scratch_shapes=[
                pltpu.VMEM((samples, local_features), jnp.bfloat16),
                pltpu.VMEM((samples // TILE, local_features, TILE), jnp.bfloat16),
                pltpu.VMEM((2, 4, targets, samples), jnp.bfloat16),
                pltpu.VMEM((targets, samples), jnp.bfloat16),
                pltpu.VMEM((targets, local_features), jnp.bfloat16),
                dma((count,)), dma,
                dma((2,)), dma((2,)), dma((2,)), dma((2,)), dma((2, count)), dma((2, count)),
            ],
            compiler_params=pltpu.CompilerParams(collective_id=0, has_side_effects=True, vmem_limit_bytes=60 * 1024 * 1024),
            name='block_lasso',
        )(x_local, coef_local.T, targets_local.T, step_local[None, :])
        return w_t.T, r_t.T

    return jax.shard_map(local_run, mesh=mesh, in_specs=(P('prob', 'feat'), P(('prob', 'feat'), None), P('prob', None), P(('prob', 'feat'))), out_specs=(P(('prob', 'feat'), None), P('prob', None)), check_vma=False)
```

```python
import functools

import jax
import jax.numpy as jnp
from jax import lax
from jax.experimental import pallas as pl
from jax.experimental.pallas import tpu as pltpu
from jax.sharding import PartitionSpec as P

SWEEPS = 6
COMBINE_WEIGHT = 0.8
RELAY_ROWS = 3072
TILE = 256
MESH = pl.DeviceIdType.MESH
OWN, PARTNER, CROSS, RELAYED = 0, 1, 2, 3


def chunk_list(samples):
    sizes = [1024] + [2048] * (samples // 2048 - 1) + [1024]
    return [(sum(sizes[:i]), size) for i, size in enumerate(sizes)]


def kernel(chunks, lasso_weight, samples, *refs):
    (x_hbm, w0_hbm, y_hbm, eta_hbm, wv, rv, xv, xt, ubuf, dwv, eta_ref, x_sem, small_sem,
     own_send, cross_send, relay_send, own_recv, cross_recv, relay_recv) = refs
    count = len(chunks)
    late = [c for c in range(count) if c % 2 == 1]
    me = lax.axis_index('feat')
    partner = me + 1 - 2 * lax.rem(me, 2)
    cross = 3 - me

    def rows_of(c):
        start, size = chunks[c]
        return pl.ds(start, size)

    def tiles_of(c):
        start, size = chunks[c]
        return range(start // TILE, (start + size) // TILE)

    def x_copy(c):
        return pltpu.make_async_copy(x_hbm.at[rows_of(c)], xv.at[rows_of(c)], x_sem.at[c])

    def w_copy():
        return pltpu.make_async_copy(w0_hbm, wv, small_sem.at[0])

    def y_copy():
        return pltpu.make_async_copy(y_hbm, rv, small_sem.at[1])

    def eta_copy():
        return pltpu.make_async_copy(eta_hbm, eta_ref, small_sem.at[2])

    def remote(par, c, src, dst, peer, send_sem, recv_sem):
        return pltpu.make_async_remote_copy(
            src_ref=ubuf.at[par, src, :, rows_of(c)], dst_ref=ubuf.at[par, dst, :, rows_of(c)],
            send_sem=send_sem.at[par, c], recv_sem=recv_sem.at[par, c], device_id={'feat': peer}, device_id_type=MESH)

    def own_copy(par, c):
        return remote(par, c, OWN, PARTNER, partner, own_send, own_recv)

    def cross_copy(par, c):
        return remote(par, c, OWN, CROSS, cross, cross_send, cross_recv)

    def relay_copy(par, c):
        return remote(par, c, CROSS, RELAYED, partner, relay_send, relay_recv)

    def transpose_x(c):
        for t in tiles_of(c):
            xt[t] = xv[pl.ds(t * TILE, TILE), :].T

    def forward(par, c, first):
        change = dwv[...]
        for t in tiles_of(c):
            rows = pl.ds(t * TILE, TILE)
            if first:
                product = lax.dot_general(change, xv[rows, :], (((1,), (1,)), ((), ())), preferred_element_type=jnp.float32)
            else:
                product = jnp.dot(change, xt[t], preferred_element_type=jnp.float32)
            ubuf[par, OWN, :, rows] = product.astype(jnp.bfloat16)
        if first and c not in late:
            transpose_x(c)

    def update_weights(gradient):
        eta = jnp.broadcast_to(eta_ref[...], gradient.shape)
        threshold = eta * lasso_weight
        weights = wv[...]
        stepped = weights + eta * (gradient * (1.0 / samples))
        shrunk = jnp.where(stepped > threshold, stepped - threshold, jnp.where(stepped < -threshold, stepped + threshold, 0.0))
        change = shrunk - weights
        wv[...] = weights + COMBINE_WEIGHT * change
        dwv[...] = change.astype(jnp.bfloat16)

    def wait_sends(par):
        for c in range(count):
            own_copy(par, c).wait_send()
            cross_copy(par, c).wait_send()
            relay_copy(par, c).wait_send()

    def phase(par, first=False, last=False):
        for c in range(count):
            if first:
                x_copy(c).wait()
            forward(par, c, first)
            if c == count // 2 and not first:
                wait_sends(1 - par)
            if first and c == 0:
                pl.semaphore_wait(barrier, 2)
            cross_copy(par, c).start()
            own_copy(par, c).start()
        if first:
            y_copy().wait()
            eta_copy().wait()
        gradient = None
        done = 0
        for step in range(count):
            cross_copy(par, step).wait_recv()
            relay_copy(par, step).start()
            if first and step in late:
                transpose_x(step)
            arrived = chunks[step][0] + chunks[step][1]
            while done < count and (step == count - 1 or chunks[done][0] + chunks[done][1] + RELAY_ROWS <= arrived):
                c = done
                done += 1
                own_copy(par, c).wait_recv()
                relay_copy(par, c).wait_recv()
                rows = rows_of(c)
                u = [ubuf[par, slot, :, rows].astype(jnp.float32) for slot in range(4)]
                total = (u[OWN] + u[PARTNER]) + (u[CROSS] + u[RELAYED])
                residual = rv[:, rows] - (total if first else COMBINE_WEIGHT * total)
                rv[:, rows] = residual
                if not last:
                    part = jnp.dot(residual.astype(jnp.bfloat16), xv[rows, :], preferred_element_type=jnp.float32)
                    gradient = part if gradient is None else gradient + part
        if not last:
            update_weights(gradient)

    w_copy().start()
    for c in range(count):
        x_copy(c).start()
        if c == 0:
            y_copy().start()
            eta_copy().start()
    barrier = pltpu.get_barrier_semaphore()
    for peer in (partner, cross):
        pl.semaphore_signal(barrier, inc=1, device_id={'feat': peer}, device_id_type=MESH)
    w_copy().wait()
    dwv[...] = wv[...].astype(jnp.bfloat16)

    phase(0, first=True)

    def sweep(s, carry):
        phase(lax.rem(s, 2))
        return carry

    lax.fori_loop(1, SWEEPS, sweep, 0)
    phase(SWEEPS % 2, last=True)
    wait_sends(SWEEPS % 2)


def solution(mesh):
    group_size = mesh.shape['feat']

    def local_run(x_local, coef_local, targets_local, step_local):
        samples, local_features = x_local.shape
        targets = coef_local.shape[1]
        features = local_features * group_size
        lasso_weight = 0.3 * group_size / features ** 0.5
        chunks = chunk_list(samples)
        count = len(chunks)
        hbm_spec = pl.BlockSpec(memory_space=pltpu.HBM)
        vmem_spec = pl.BlockSpec(memory_space=pltpu.VMEM)
        dma = pltpu.SemaphoreType.DMA
        w_t, r_t = pl.pallas_call(
            functools.partial(kernel, chunks, lasso_weight, samples),
            out_shape=(pltpu.VMEM((targets, local_features), jnp.float32), pltpu.VMEM((targets, samples), jnp.float32)),
            in_specs=[hbm_spec] * 4,
            out_specs=(vmem_spec, vmem_spec),
            scratch_shapes=[
                pltpu.VMEM((samples, local_features), jnp.bfloat16),
                pltpu.VMEM((samples // TILE, local_features, TILE), jnp.bfloat16),
                pltpu.VMEM((2, 4, targets, samples), jnp.bfloat16),
                pltpu.VMEM((targets, local_features), jnp.bfloat16),
                pltpu.VMEM((1, local_features), jnp.float32),
                dma((count,)), dma((3,)),
                dma((2, count)), dma((2, count)), dma((2, count)), dma((2, count)), dma((2, count)), dma((2, count)),
            ],
            compiler_params=pltpu.CompilerParams(collective_id=0, has_side_effects=True, vmem_limit_bytes=60 * 1024 * 1024),
            name='block_lasso',
        )(x_local, coef_local.T, targets_local.T, step_local[None, :])
        return w_t.T, r_t.T

    return jax.shard_map(local_run, mesh=mesh, in_specs=(P('prob', 'feat'), P(('prob', 'feat'), None), P('prob', None), P(('prob', 'feat'))), out_specs=(P(('prob', 'feat'), None), P('prob', None)), check_vma=False)
```

```python
import functools

import jax
import jax.numpy as jnp
from jax import lax
from jax.experimental import pallas as pl
from jax.experimental.pallas import tpu as pltpu
from jax.sharding import PartitionSpec as P

SWEEPS = 6
COMBINE_WEIGHT = 0.8
RELAY_ROWS = 3072
TILE = 256
MESH = pl.DeviceIdType.MESH
OWN, PARTNER, CROSS, RELAYED = 0, 1, 2, 3


def chunk_list(samples):
    sizes = [2048] * (samples // 2048)
    return [(sum(sizes[:i]), size) for i, size in enumerate(sizes)]


def kernel(chunks, lasso_weight, samples, *refs):
    (x_hbm, w0_hbm, y_hbm, eta_hbm, wv, rv, xv, xt, ubuf, dwv, eta_ref, x_sem, small_sem,
     own_send, cross_send, relay_send, own_recv, cross_recv, relay_recv) = refs
    count = len(chunks)
    late = [c for c in range(count) if c % 2 == 1]
    me = lax.axis_index('feat')
    partner = me + 1 - 2 * lax.rem(me, 2)
    cross = 3 - me

    def rows_of(c):
        start, size = chunks[c]
        return pl.ds(start, size)

    def tiles_of(c):
        start, size = chunks[c]
        return range(start // TILE, (start + size) // TILE)

    def x_copy(c):
        return pltpu.make_async_copy(x_hbm.at[rows_of(c)], xv.at[rows_of(c)], x_sem.at[c])

    def w_copy():
        return pltpu.make_async_copy(w0_hbm, wv, small_sem.at[0])

    def y_copy():
        return pltpu.make_async_copy(y_hbm, rv, small_sem.at[1])

    def eta_copy():
        return pltpu.make_async_copy(eta_hbm, eta_ref, small_sem.at[2])

    def remote(par, c, src, dst, peer, send_sem, recv_sem):
        return pltpu.make_async_remote_copy(
            src_ref=ubuf.at[par, src, :, rows_of(c)], dst_ref=ubuf.at[par, dst, :, rows_of(c)],
            send_sem=send_sem.at[par, c], recv_sem=recv_sem.at[par, c], device_id={'feat': peer}, device_id_type=MESH)

    def own_copy(par, c):
        return remote(par, c, OWN, PARTNER, partner, own_send, own_recv)

    def cross_copy(par, c):
        return remote(par, c, OWN, CROSS, cross, cross_send, cross_recv)

    def relay_copy(par, c):
        return remote(par, c, CROSS, RELAYED, partner, relay_send, relay_recv)

    def transpose_x(c):
        for t in tiles_of(c):
            xt[t] = xv[pl.ds(t * TILE, TILE), :].T

    def forward(par, c, first):
        change = dwv[...]
        for t in tiles_of(c):
            rows = pl.ds(t * TILE, TILE)
            if first:
                product = lax.dot_general(change, xv[rows, :], (((1,), (1,)), ((), ())), preferred_element_type=jnp.float32)
            else:
                product = jnp.dot(change, xt[t], preferred_element_type=jnp.float32)
            ubuf[par, OWN, :, rows] = product.astype(jnp.bfloat16)
        if first and c not in late:
            transpose_x(c)

    def update_weights(gradient):
        eta = jnp.broadcast_to(eta_ref[...], gradient.shape)
        threshold = eta * lasso_weight
        weights = wv[...]
        stepped = weights + eta * (gradient * (1.0 / samples))
        shrunk = jnp.where(stepped > threshold, stepped - threshold, jnp.where(stepped < -threshold, stepped + threshold, 0.0))
        change = shrunk - weights
        wv[...] = weights + COMBINE_WEIGHT * change
        dwv[...] = change.astype(jnp.bfloat16)

    def wait_sends(par):
        for c in range(count):
            own_copy(par, c).wait_send()
            cross_copy(par, c).wait_send()
            relay_copy(par, c).wait_send()

    def phase(par, first=False, last=False):
        for c in range(count):
            if first:
                x_copy(c).wait()
            forward(par, c, first)
            if c == count // 2 and not first:
                wait_sends(1 - par)
            if first and c == 0:
                pl.semaphore_wait(barrier, 2)
            cross_copy(par, c).start()
            own_copy(par, c).start()
        if first:
            y_copy().wait()
            eta_copy().wait()
        gradient = None
        done = 0
        for step in range(count):
            cross_copy(par, step).wait_recv()
            relay_copy(par, step).start()
            if first and step in late:
                transpose_x(step)
            arrived = chunks[step][0] + chunks[step][1]
            while done < count and (step == count - 1 or chunks[done][0] + chunks[done][1] + RELAY_ROWS <= arrived):
                c = done
                done += 1
                own_copy(par, c).wait_recv()
                relay_copy(par, c).wait_recv()
                rows = rows_of(c)
                u = [ubuf[par, slot, :, rows].astype(jnp.float32) for slot in range(4)]
                total = (u[OWN] + u[PARTNER]) + (u[CROSS] + u[RELAYED])
                residual = rv[:, rows] - (total if first else COMBINE_WEIGHT * total)
                rv[:, rows] = residual
                if not last:
                    part = jnp.dot(residual.astype(jnp.bfloat16), xv[rows, :], preferred_element_type=jnp.float32)
                    gradient = part if gradient is None else gradient + part
        if not last:
            update_weights(gradient)

    w_copy().start()
    for c in range(count):
        x_copy(c).start()
        if c == 0:
            y_copy().start()
            eta_copy().start()
    barrier = pltpu.get_barrier_semaphore()
    for peer in (partner, cross):
        pl.semaphore_signal(barrier, inc=1, device_id={'feat': peer}, device_id_type=MESH)
    w_copy().wait()
    dwv[...] = wv[...].astype(jnp.bfloat16)

    phase(0, first=True)

    def sweep(s, carry):
        phase(lax.rem(s, 2))
        return carry

    lax.fori_loop(1, SWEEPS, sweep, 0)
    phase(SWEEPS % 2, last=True)
    wait_sends(SWEEPS % 2)


def solution(mesh):
    group_size = mesh.shape['feat']

    def local_run(x_local, coef_local, targets_local, step_local):
        samples, local_features = x_local.shape
        targets = coef_local.shape[1]
        features = local_features * group_size
        lasso_weight = 0.3 * group_size / features ** 0.5
        chunks = chunk_list(samples)
        count = len(chunks)
        hbm_spec = pl.BlockSpec(memory_space=pltpu.HBM)
        vmem_spec = pl.BlockSpec(memory_space=pltpu.VMEM)
        dma = pltpu.SemaphoreType.DMA
        w_t, r_t = pl.pallas_call(
            functools.partial(kernel, chunks, lasso_weight, samples),
            out_shape=(pltpu.VMEM((targets, local_features), jnp.float32), pltpu.VMEM((targets, samples), jnp.float32)),
            in_specs=[hbm_spec] * 4,
            out_specs=(vmem_spec, vmem_spec),
            scratch_shapes=[
                pltpu.VMEM((samples, local_features), jnp.bfloat16),
                pltpu.VMEM((samples // TILE, local_features, TILE), jnp.bfloat16),
                pltpu.VMEM((2, 4, targets, samples), jnp.bfloat16),
                pltpu.VMEM((targets, local_features), jnp.bfloat16),
                pltpu.VMEM((1, local_features), jnp.float32),
                dma((count,)), dma((3,)),
                dma((2, count)), dma((2, count)), dma((2, count)), dma((2, count)), dma((2, count)), dma((2, count)),
            ],
            compiler_params=pltpu.CompilerParams(collective_id=0, has_side_effects=True, vmem_limit_bytes=60 * 1024 * 1024),
            name='block_lasso',
        )(x_local, coef_local.T, targets_local.T, step_local[None, :])
        return w_t.T, r_t.T

    return jax.shard_map(local_run, mesh=mesh, in_specs=(P('prob', 'feat'), P(('prob', 'feat'), None), P('prob', None), P(('prob', 'feat'))), out_specs=(P(('prob', 'feat'), None), P('prob', None)), check_vma=False)
```

```python
import functools

import jax
import jax.numpy as jnp
from jax import lax
from jax.experimental import pallas as pl
from jax.experimental.pallas import tpu as pltpu
from jax.sharding import PartitionSpec as P

SWEEPS = 6
COMBINE_WEIGHT = 0.8
RELAY_ROWS = 3072
TILE = 256
MESH = pl.DeviceIdType.MESH
OWN, PARTNER, CROSS, RELAYED = 0, 1, 2, 3


def chunk_list(samples):
    sizes = [2048] * (samples // 2048)
    return [(sum(sizes[:i]), size) for i, size in enumerate(sizes)]


def kernel(chunks, lasso_weight, samples, *refs):
    (x_hbm, w0_hbm, y_hbm, eta_hbm, wv, rv, xv, xt, ubuf, dwv, eta_ref, x_sem, small_sem,
     own_send, cross_send, relay_send, own_recv, cross_recv, relay_recv) = refs
    count = len(chunks)
    me = lax.axis_index('feat')
    partner = me + 1 - 2 * lax.rem(me, 2)
    cross = 3 - me

    def rows_of(c):
        start, size = chunks[c]
        return pl.ds(start, size)

    def tiles_of(c):
        start, size = chunks[c]
        return range(start // TILE, (start + size) // TILE)

    def x_copy(c):
        return pltpu.make_async_copy(x_hbm.at[rows_of(c)], xv.at[rows_of(c)], x_sem.at[c])

    def w_copy():
        return pltpu.make_async_copy(w0_hbm, wv, small_sem.at[0])

    def y_copy():
        return pltpu.make_async_copy(y_hbm, rv, small_sem.at[1])

    def eta_copy():
        return pltpu.make_async_copy(eta_hbm, eta_ref, small_sem.at[2])

    def remote(par, c, src, dst, peer, send_sem, recv_sem):
        return pltpu.make_async_remote_copy(
            src_ref=ubuf.at[par, src, :, rows_of(c)], dst_ref=ubuf.at[par, dst, :, rows_of(c)],
            send_sem=send_sem.at[par, c], recv_sem=recv_sem.at[par, c], device_id={'feat': peer}, device_id_type=MESH)

    def own_copy(par, c):
        return remote(par, c, OWN, PARTNER, partner, own_send, own_recv)

    def cross_copy(par, c):
        return remote(par, c, OWN, CROSS, cross, cross_send, cross_recv)

    def relay_copy(par, c):
        return remote(par, c, CROSS, RELAYED, partner, relay_send, relay_recv)

    def forward(par, c, first):
        change = dwv[...]
        for t in tiles_of(c):
            rows = pl.ds(t * TILE, TILE)
            if first:
                x_t = xv[rows, :].T
                xt[t] = x_t
            else:
                x_t = xt[t]
            product = jnp.dot(change, x_t, preferred_element_type=jnp.float32)
            ubuf[par, OWN, :, rows] = product.astype(jnp.bfloat16)

    def update_weights(gradient):
        eta = jnp.broadcast_to(eta_ref[...], gradient.shape)
        threshold = eta * lasso_weight
        weights = wv[...]
        stepped = weights + eta * (gradient * (1.0 / samples))
        shrunk = jnp.where(stepped > threshold, stepped - threshold, jnp.where(stepped < -threshold, stepped + threshold, 0.0))
        change = shrunk - weights
        wv[...] = weights + COMBINE_WEIGHT * change
        dwv[...] = change.astype(jnp.bfloat16)

    def wait_sends(par):
        for c in range(count):
            own_copy(par, c).wait_send()
            cross_copy(par, c).wait_send()
            relay_copy(par, c).wait_send()

    def phase(par, first=False, last=False):
        for c in range(count):
            if first:
                x_copy(c).wait()
            forward(par, c, first)
            if c == count // 2 and not first:
                wait_sends(1 - par)
            if first and c == 0:
                pl.semaphore_wait(barrier, 2)
            cross_copy(par, c).start()
            own_copy(par, c).start()
        if first:
            y_copy().wait()
            eta_copy().wait()
        gradient = None
        done = 0
        for step in range(count):
            cross_copy(par, step).wait_recv()
            relay_copy(par, step).start()
            arrived = chunks[step][0] + chunks[step][1]
            while done < count and (step == count - 1 or chunks[done][0] + chunks[done][1] + RELAY_ROWS <= arrived):
                c = done
                done += 1
                own_copy(par, c).wait_recv()
                relay_copy(par, c).wait_recv()
                rows = rows_of(c)
                u = [ubuf[par, slot, :, rows].astype(jnp.float32) for slot in range(4)]
                total = (u[OWN] + u[PARTNER]) + (u[CROSS] + u[RELAYED])
                residual = rv[:, rows] - (total if first else COMBINE_WEIGHT * total)
                rv[:, rows] = residual
                if not last:
                    part = jnp.dot(residual.astype(jnp.bfloat16), xv[rows, :], preferred_element_type=jnp.float32)
                    gradient = part if gradient is None else gradient + part
        if not last:
            update_weights(gradient)

    w_copy().start()
    for c in range(count):
        x_copy(c).start()
        if c == 0:
            y_copy().start()
            eta_copy().start()
    barrier = pltpu.get_barrier_semaphore()
    for peer in (partner, cross):
        pl.semaphore_signal(barrier, inc=1, device_id={'feat': peer}, device_id_type=MESH)
    w_copy().wait()
    dwv[...] = wv[...].astype(jnp.bfloat16)

    phase(0, first=True)

    def sweep(s, carry):
        phase(lax.rem(s, 2))
        return carry

    lax.fori_loop(1, SWEEPS, sweep, 0)
    phase(SWEEPS % 2, last=True)
    wait_sends(SWEEPS % 2)


def solution(mesh):
    group_size = mesh.shape['feat']

    def local_run(x_local, coef_local, targets_local, step_local):
        samples, local_features = x_local.shape
        targets = coef_local.shape[1]
        features = local_features * group_size
        lasso_weight = 0.3 * group_size / features ** 0.5
        chunks = chunk_list(samples)
        count = len(chunks)
        hbm_spec = pl.BlockSpec(memory_space=pltpu.HBM)
        vmem_spec = pl.BlockSpec(memory_space=pltpu.VMEM)
        dma = pltpu.SemaphoreType.DMA
        w_t, r_t = pl.pallas_call(
            functools.partial(kernel, chunks, lasso_weight, samples),
            out_shape=(pltpu.VMEM((targets, local_features), jnp.float32), pltpu.VMEM((targets, samples), jnp.float32)),
            in_specs=[hbm_spec] * 4,
            out_specs=(vmem_spec, vmem_spec),
            scratch_shapes=[
                pltpu.VMEM((samples, local_features), jnp.bfloat16),
                pltpu.VMEM((samples // TILE, local_features, TILE), jnp.bfloat16),
                pltpu.VMEM((2, 4, targets, samples), jnp.bfloat16),
                pltpu.VMEM((targets, local_features), jnp.bfloat16),
                pltpu.VMEM((1, local_features), jnp.float32),
                dma((count,)), dma((3,)),
                dma((2, count)), dma((2, count)), dma((2, count)), dma((2, count)), dma((2, count)), dma((2, count)),
            ],
            compiler_params=pltpu.CompilerParams(collective_id=0, has_side_effects=True, vmem_limit_bytes=60 * 1024 * 1024),
            name='block_lasso',
        )(x_local, coef_local.T, targets_local.T, step_local[None, :])
        return w_t.T, r_t.T

    return jax.shard_map(local_run, mesh=mesh, in_specs=(P('prob', 'feat'), P(('prob', 'feat'), None), P('prob', None), P(('prob', 'feat'))), out_specs=(P(('prob', 'feat'), None), P('prob', None)), check_vma=False)
```

```python
import functools

import jax
import jax.numpy as jnp
from jax import lax
from jax.experimental import pallas as pl
from jax.experimental.pallas import tpu as pltpu
from jax.sharding import PartitionSpec as P

SWEEPS = 6
COMBINE_WEIGHT = 0.8
LAG = 2
TILE = 256
MESH = pl.DeviceIdType.MESH
OWN, PARTNER, CROSS, RELAYED = 0, 1, 2, 3


def chunk_list(samples):
    size = samples // 8
    return [(i * size, size) for i in range(8)]


def kernel(chunks, lasso_weight, samples, *refs):
    (x_hbm, w0_ref, y_hbm, eta_ref, wv, rv, xv, xt, ubuf, dwv, x_sem, y_sem,
     own_send, cross_send, relay_send, own_recv, cross_recv, relay_recv) = refs
    count = len(chunks)
    targets = w0_ref.shape[0]
    me = lax.axis_index('feat')
    partner = me + 1 - 2 * lax.rem(me, 2)
    cross = 3 - me

    def rows_of(c):
        start, size = chunks[c]
        return pl.ds(start, size)

    def tiles_of(c):
        start, size = chunks[c]
        return range(start // TILE, (start + size) // TILE)

    def x_copy(c):
        return pltpu.make_async_copy(x_hbm.at[rows_of(c)], xv.at[rows_of(c)], x_sem.at[c])

    def remote(par, c, src, dst, peer, send_sem, recv_sem):
        return pltpu.make_async_remote_copy(
            src_ref=ubuf.at[par, src, :, rows_of(c)], dst_ref=ubuf.at[par, dst, :, rows_of(c)],
            send_sem=send_sem.at[par, c], recv_sem=recv_sem.at[par, c], device_id={'feat': peer}, device_id_type=MESH)

    def own_copy(par, c):
        return remote(par, c, OWN, PARTNER, partner, own_send, own_recv)

    def cross_copy(par, c):
        return remote(par, c, OWN, CROSS, cross, cross_send, cross_recv)

    def relay_copy(par, c):
        return remote(par, c, CROSS, RELAYED, partner, relay_send, relay_recv)

    def forward(par, c, first):
        change = dwv[...]
        for t in tiles_of(c):
            rows = pl.ds(t * TILE, TILE)
            if first:
                x_t = xv[rows, :].T
                xt[t] = x_t
            else:
                x_t = xt[t]
            product = jnp.dot(change, x_t, preferred_element_type=jnp.float32)
            ubuf[par, OWN, :, rows] = product.astype(jnp.bfloat16)

    def update_weights(gradient):
        eta = jnp.broadcast_to(eta_ref[...], gradient.shape)
        threshold = eta * lasso_weight
        weights = wv[...]
        stepped = weights + eta * (gradient * (1.0 / samples))
        shrunk = jnp.where(stepped > threshold, stepped - threshold, jnp.where(stepped < -threshold, stepped + threshold, 0.0))
        change = shrunk - weights
        wv[...] = weights + COMBINE_WEIGHT * change
        dwv[...] = change.astype(jnp.bfloat16)

    def wait_sends(par):
        for c in range(count):
            own_copy(par, c).wait_send()
            cross_copy(par, c).wait_send()
            relay_copy(par, c).wait_send()

    def phase(par, first=False, last=False):
        for c in range(count):
            if first:
                x_copy(c).wait()
            forward(par, c, first)
            if c == count // 2 and not first:
                wait_sends(1 - par)
            if first and c == 0:
                pl.semaphore_wait(barrier, 2)
            cross_copy(par, c).start()
            own_copy(par, c).start()
        if first:
            pltpu.make_async_copy(y_hbm, rv, y_sem).wait()
        gradient = None
        for step in range(count + LAG):
            if step < count:
                cross_copy(par, step).wait_recv()
                relay_copy(par, step).start()
            c = step - LAG
            if c < 0:
                continue
            own_copy(par, c).wait_recv()
            relay_copy(par, c).wait_recv()
            rows = rows_of(c)
            u = [ubuf[par, slot, :, rows].astype(jnp.float32) for slot in range(4)]
            total = (u[OWN] + u[PARTNER]) + (u[CROSS] + u[RELAYED])
            residual = rv[:, rows] - (total if first else COMBINE_WEIGHT * total)
            rv[:, rows] = residual
            if not last:
                part = jnp.dot(residual.astype(jnp.bfloat16), xv[rows, :], preferred_element_type=jnp.float32)
                gradient = part if gradient is None else gradient + part
        if not last:
            update_weights(gradient)

    for c in range(count):
        x_copy(c).start()
        if c == 0:
            pltpu.make_async_copy(y_hbm, rv, y_sem).start()
    barrier = pltpu.get_barrier_semaphore()
    for peer in (partner, cross):
        pl.semaphore_signal(barrier, inc=1, device_id={'feat': peer}, device_id_type=MESH)
    wv[...] = w0_ref[...]
    dwv[...] = w0_ref[...].astype(jnp.bfloat16)
    phase(0, first=True)

    def sweep(s, carry):
        phase(lax.rem(s, 2))
        return carry

    lax.fori_loop(1, SWEEPS, sweep, 0)
    phase(SWEEPS % 2, last=True)
    wait_sends(SWEEPS % 2)


def leave(w_ref, r_ref, w_hbm, r_hbm, sem):
    copies = [pltpu.make_async_copy(w_ref, w_hbm, sem.at[0]), pltpu.make_async_copy(r_ref, r_hbm, sem.at[1])]
    for copy in copies:
        copy.start()
    for copy in copies:
        copy.wait()


def solution(mesh):
    group_size = mesh.shape['feat']

    def local_run(x_local, coef_local, targets_local, step_local):
        samples, local_features = x_local.shape
        targets = coef_local.shape[1]
        features = local_features * group_size
        lasso_weight = 0.3 * group_size / features ** 0.5
        chunks = chunk_list(samples)
        count = len(chunks)
        any_spec = pl.BlockSpec(memory_space=pl.ANY)
        vmem_spec = pl.BlockSpec(memory_space=pltpu.VMEM)
        dma = pltpu.SemaphoreType.DMA
        w_t, r_t = pl.pallas_call(
            functools.partial(kernel, chunks, lasso_weight, samples),
            out_shape=(pltpu.VMEM((targets, local_features), jnp.float32), pltpu.VMEM((targets, samples), jnp.float32)),
            in_specs=[pl.BlockSpec(memory_space=pltpu.HBM), vmem_spec, pl.BlockSpec(memory_space=pltpu.HBM), vmem_spec],
            out_specs=(vmem_spec, vmem_spec),
            scratch_shapes=[
                pltpu.VMEM((samples, local_features), jnp.bfloat16),
                pltpu.VMEM((samples // TILE, local_features, TILE), jnp.bfloat16),
                pltpu.VMEM((2, 4, targets, samples), jnp.bfloat16),
                pltpu.VMEM((targets, local_features), jnp.bfloat16),
                dma((count,)), dma,
                dma((2, count)), dma((2, count)), dma((2, count)), dma((2, count)), dma((2, count)), dma((2, count)),
            ],
            compiler_params=pltpu.CompilerParams(collective_id=0, has_side_effects=True, vmem_limit_bytes=60 * 1024 * 1024),
            name='block_lasso',
        )(x_local, coef_local.T, targets_local.T, step_local[None, :])
        w_t, r_t = pl.pallas_call(
            leave,
            out_shape=(jax.ShapeDtypeStruct(w_t.shape, w_t.dtype), jax.ShapeDtypeStruct(r_t.shape, r_t.dtype)),
            in_specs=[vmem_spec, vmem_spec],
            out_specs=(any_spec, any_spec),
            scratch_shapes=[dma((2,))],
            name='leave',
        )(w_t, r_t)
        return w_t.T, r_t.T

    return jax.shard_map(local_run, mesh=mesh, in_specs=(P('prob', 'feat'), P(('prob', 'feat'), None), P('prob', None), P(('prob', 'feat'))), out_specs=(P(('prob', 'feat'), None), P('prob', None)), check_vma=False)
```

```python
import functools

import jax
import jax.numpy as jnp
from jax import lax
from jax.experimental import pallas as pl
from jax.experimental.pallas import tpu as pltpu
from jax.sharding import PartitionSpec as P

SWEEPS = 6
COMBINE_WEIGHT = 0.8
LAG = 2
TILE = 256
MESH = pl.DeviceIdType.MESH
OWN, PARTNER, CROSS, RELAYED = 0, 1, 2, 3


def chunk_list(samples):
    size = samples // 8
    return [(i * size, size) for i in range(8)]


def kernel(chunks, lasso_weight, samples, *refs):
    (x_hbm, w0_ref, y_hbm, eta_ref, wv, rv, xv, xt, ubuf, dwv, x_sem, y_sem,
     own_send, cross_send, relay_send, own_recv, cross_recv, relay_recv) = refs
    count = len(chunks)
    targets = w0_ref.shape[0]
    me = lax.axis_index('feat')
    partner = me + 1 - 2 * lax.rem(me, 2)
    cross = 3 - me

    def rows_of(c):
        start, size = chunks[c]
        return pl.ds(start, size)

    def tiles_of(c):
        start, size = chunks[c]
        return range(start // TILE, (start + size) // TILE)

    def x_copy(c):
        return pltpu.make_async_copy(x_hbm.at[rows_of(c)], xv.at[rows_of(c)], x_sem.at[c])

    def remote(par, c, src, dst, peer, send_sem, recv_sem):
        return pltpu.make_async_remote_copy(
            src_ref=ubuf.at[par, src, :, rows_of(c)], dst_ref=ubuf.at[par, dst, :, rows_of(c)],
            send_sem=send_sem.at[par, c], recv_sem=recv_sem.at[par, c], device_id={'feat': peer}, device_id_type=MESH)

    def own_copy(par, c):
        return remote(par, c, OWN, PARTNER, partner, own_send, own_recv)

    def cross_copy(par, c):
        return remote(par, c, OWN, CROSS, cross, cross_send, cross_recv)

    def relay_copy(par, c):
        return remote(par, c, CROSS, RELAYED, partner, relay_send, relay_recv)

    def forward(par, c, first):
        change = dwv[...]
        for t in tiles_of(c):
            rows = pl.ds(t * TILE, TILE)
            if first:
                product = lax.dot_general(change, xv[rows, :], (((1,), (1,)), ((), ())), preferred_element_type=jnp.float32)
                xt[t] = xv[rows, :].T
            else:
                product = jnp.dot(change, xt[t], preferred_element_type=jnp.float32)
            ubuf[par, OWN, :, rows] = product.astype(jnp.bfloat16)

    def update_weights(gradient):
        eta = jnp.broadcast_to(eta_ref[...], gradient.shape)
        threshold = eta * lasso_weight
        weights = wv[...]
        stepped = weights + eta * (gradient * (1.0 / samples))
        shrunk = jnp.where(stepped > threshold, stepped - threshold, jnp.where(stepped < -threshold, stepped + threshold, 0.0))
        change = shrunk - weights
        wv[...] = weights + COMBINE_WEIGHT * change
        dwv[...] = change.astype(jnp.bfloat16)

    def wait_sends(par):
        for c in range(count):
            own_copy(par, c).wait_send()
            cross_copy(par, c).wait_send()
            relay_copy(par, c).wait_send()

    def phase(par, first=False, last=False):
        for c in range(count):
            if first:
                x_copy(c).wait()
            forward(par, c, first)
            if c == count // 2 and not first:
                wait_sends(1 - par)
            cross_copy(par, c).start()
            own_copy(par, c).start()
        if first:
            pltpu.make_async_copy(y_hbm, rv, y_sem).wait()
        gradient = None
        for step in range(count + LAG):
            if step < count:
                cross_copy(par, step).wait_recv()
                relay_copy(par, step).start()
            c = step - LAG
            if c < 0:
                continue
            own_copy(par, c).wait_recv()
            relay_copy(par, c).wait_recv()
            rows = rows_of(c)
            u = [ubuf[par, slot, :, rows].astype(jnp.float32) for slot in range(4)]
            total = (u[OWN] + u[PARTNER]) + (u[CROSS] + u[RELAYED])
            residual = rv[:, rows] - (total if first else COMBINE_WEIGHT * total)
            rv[:, rows] = residual
            if not last:
                part = jnp.dot(residual.astype(jnp.bfloat16), xv[rows, :], preferred_element_type=jnp.float32)
                gradient = part if gradient is None else gradient + part
        if not last:
            update_weights(gradient)

    for c in range(count):
        x_copy(c).start()
        if c == 0:
            pltpu.make_async_copy(y_hbm, rv, y_sem).start()
    barrier = pltpu.get_barrier_semaphore()
    for peer in (partner, cross):
        pl.semaphore_signal(barrier, inc=1, device_id={'feat': peer}, device_id_type=MESH)
    wv[...] = w0_ref[...]
    dwv[...] = w0_ref[...].astype(jnp.bfloat16)
    pl.semaphore_wait(barrier, 2)

    phase(0, first=True)

    def sweep(s, carry):
        phase(lax.rem(s, 2))
        return carry

    lax.fori_loop(1, SWEEPS, sweep, 0)
    phase(SWEEPS % 2, last=True)
    wait_sends(SWEEPS % 2)


def solution(mesh):
    group_size = mesh.shape['feat']

    def local_run(x_local, coef_local, targets_local, step_local):
        samples, local_features = x_local.shape
        targets = coef_local.shape[1]
        features = local_features * group_size
        lasso_weight = 0.3 * group_size / features ** 0.5
        chunks = chunk_list(samples)
        count = len(chunks)
        any_spec = pl.BlockSpec(memory_space=pl.ANY)
        vmem_spec = pl.BlockSpec(memory_space=pltpu.VMEM)
        dma = pltpu.SemaphoreType.DMA
        w_t, r_t = pl.pallas_call(
            functools.partial(kernel, chunks, lasso_weight, samples),
            out_shape=(pltpu.VMEM((targets, local_features), jnp.float32), pltpu.VMEM((targets, samples), jnp.float32)),
            in_specs=[pl.BlockSpec(memory_space=pltpu.HBM), vmem_spec, pl.BlockSpec(memory_space=pltpu.HBM), vmem_spec],
            out_specs=(vmem_spec, vmem_spec),
            scratch_shapes=[
                pltpu.VMEM((samples, local_features), jnp.bfloat16),
                pltpu.VMEM((samples // TILE, local_features, TILE), jnp.bfloat16),
                pltpu.VMEM((2, 4, targets, samples), jnp.bfloat16),
                pltpu.VMEM((targets, local_features), jnp.bfloat16),
                dma((count,)), dma,
                dma((2, count)), dma((2, count)), dma((2, count)), dma((2, count)), dma((2, count)), dma((2, count)),
            ],
            compiler_params=pltpu.CompilerParams(collective_id=0, has_side_effects=True, vmem_limit_bytes=60 * 1024 * 1024),
            name='block_lasso',
        )(x_local, coef_local.T, targets_local.T, step_local[None, :])
        return w_t.T, r_t.T

    return jax.shard_map(local_run, mesh=mesh, in_specs=(P('prob', 'feat'), P(('prob', 'feat'), None), P('prob', None), P(('prob', 'feat'))), out_specs=(P(('prob', 'feat'), None), P('prob', None)), check_vma=False)
```

```python
import functools

import jax
import jax.numpy as jnp
from jax import lax
from jax.experimental import pallas as pl
from jax.experimental.pallas import tpu as pltpu
from jax.sharding import PartitionSpec as P

SWEEPS = 6
COMBINE_WEIGHT = 0.8
LAG = 2
TILE = 256
MESH = pl.DeviceIdType.MESH
OWN, PARTNER, CROSS, RELAYED = 0, 1, 2, 3


def chunk_list(samples):
    sizes = [2048] * (samples // 2048 - 1) + [1024, 1024]
    return [(sum(sizes[:i]), size) for i, size in enumerate(sizes)]


def kernel(chunks, lasso_weight, samples, *refs):
    (x_hbm, w0_ref, y_hbm, eta_ref, wv, rv, xv, xt, ubuf, dwv, x_sem, y_sem,
     own_send, cross_send, relay_send, own_recv, cross_recv, relay_recv) = refs
    count = len(chunks)
    targets = w0_ref.shape[0]
    me = lax.axis_index('feat')
    partner = me + 1 - 2 * lax.rem(me, 2)
    cross = 3 - me

    def rows_of(c):
        start, size = chunks[c]
        return pl.ds(start, size)

    def tiles_of(c):
        start, size = chunks[c]
        return range(start // TILE, (start + size) // TILE)

    def x_copy(c):
        return pltpu.make_async_copy(x_hbm.at[rows_of(c)], xv.at[rows_of(c)], x_sem.at[c])

    def remote(par, c, src, dst, peer, send_sem, recv_sem):
        return pltpu.make_async_remote_copy(
            src_ref=ubuf.at[par, src, :, rows_of(c)], dst_ref=ubuf.at[par, dst, :, rows_of(c)],
            send_sem=send_sem.at[par, c], recv_sem=recv_sem.at[par, c], device_id={'feat': peer}, device_id_type=MESH)

    def own_copy(par, c):
        return remote(par, c, OWN, PARTNER, partner, own_send, own_recv)

    def cross_copy(par, c):
        return remote(par, c, OWN, CROSS, cross, cross_send, cross_recv)

    def relay_copy(par, c):
        return remote(par, c, CROSS, RELAYED, partner, relay_send, relay_recv)

    def forward(par, c, first):
        change = dwv[...]
        for t in tiles_of(c):
            rows = pl.ds(t * TILE, TILE)
            if first:
                product = lax.dot_general(change, xv[rows, :], (((1,), (1,)), ((), ())), preferred_element_type=jnp.float32)
                xt[t] = xv[rows, :].T
            else:
                product = jnp.dot(change, xt[t], preferred_element_type=jnp.float32)
            ubuf[par, OWN, :, rows] = product.astype(jnp.bfloat16)

    def update_weights(gradient):
        eta = jnp.broadcast_to(eta_ref[...], gradient.shape)
        threshold = eta * lasso_weight
        weights = wv[...]
        stepped = weights + eta * (gradient * (1.0 / samples))
        shrunk = jnp.where(stepped > threshold, stepped - threshold, jnp.where(stepped < -threshold, stepped + threshold, 0.0))
        change = shrunk - weights
        wv[...] = weights + COMBINE_WEIGHT * change
        dwv[...] = change.astype(jnp.bfloat16)

    def wait_sends(par):
        for c in range(count):
            own_copy(par, c).wait_send()
            cross_copy(par, c).wait_send()
            relay_copy(par, c).wait_send()

    def phase(par, first=False, last=False):
        for c in range(count):
            if first:
                x_copy(c).wait()
            forward(par, c, first)
            if c == count // 2 and not first:
                wait_sends(1 - par)
            cross_copy(par, c).start()
            own_copy(par, c).start()
        if first:
            pltpu.make_async_copy(y_hbm, rv, y_sem).wait()
        gradient = None
        for step in range(count + LAG):
            if step < count:
                cross_copy(par, step).wait_recv()
                relay_copy(par, step).start()
            c = step - LAG
            if c < 0:
                continue
            own_copy(par, c).wait_recv()
            relay_copy(par, c).wait_recv()
            rows = rows_of(c)
            u = [ubuf[par, slot, :, rows].astype(jnp.float32) for slot in range(4)]
            total = (u[OWN] + u[PARTNER]) + (u[CROSS] + u[RELAYED])
            residual = rv[:, rows] - (total if first else COMBINE_WEIGHT * total)
            rv[:, rows] = residual
            if not last:
                part = jnp.dot(residual.astype(jnp.bfloat16), xv[rows, :], preferred_element_type=jnp.float32)
                gradient = part if gradient is None else gradient + part
        if not last:
            update_weights(gradient)

    for c in range(count):
        x_copy(c).start()
    pltpu.make_async_copy(y_hbm, rv, y_sem).start()
    barrier = pltpu.get_barrier_semaphore()
    for peer in (partner, cross):
        pl.semaphore_signal(barrier, inc=1, device_id={'feat': peer}, device_id_type=MESH)
    wv[...] = w0_ref[...]
    dwv[...] = w0_ref[...].astype(jnp.bfloat16)
    pl.semaphore_wait(barrier, 2)

    phase(0, first=True)

    def sweep(s, carry):
        phase(lax.rem(s, 2))
        return carry

    lax.fori_loop(1, SWEEPS, sweep, 0)
    phase(SWEEPS % 2, last=True)
    wait_sends(SWEEPS % 2)


def solution(mesh):
    group_size = mesh.shape['feat']

    def local_run(x_local, coef_local, targets_local, step_local):
        samples, local_features = x_local.shape
        targets = coef_local.shape[1]
        features = local_features * group_size
        lasso_weight = 0.3 * group_size / features ** 0.5
        chunks = chunk_list(samples)
        count = len(chunks)
        any_spec = pl.BlockSpec(memory_space=pl.ANY)
        vmem_spec = pl.BlockSpec(memory_space=pltpu.VMEM)
        dma = pltpu.SemaphoreType.DMA
        w_t, r_t = pl.pallas_call(
            functools.partial(kernel, chunks, lasso_weight, samples),
            out_shape=(pltpu.VMEM((targets, local_features), jnp.float32), pltpu.VMEM((targets, samples), jnp.float32)),
            in_specs=[pl.BlockSpec(memory_space=pltpu.HBM), vmem_spec, pl.BlockSpec(memory_space=pltpu.HBM), vmem_spec],
            out_specs=(vmem_spec, vmem_spec),
            scratch_shapes=[
                pltpu.VMEM((samples, local_features), jnp.bfloat16),
                pltpu.VMEM((samples // TILE, local_features, TILE), jnp.bfloat16),
                pltpu.VMEM((2, 4, targets, samples), jnp.bfloat16),
                pltpu.VMEM((targets, local_features), jnp.bfloat16),
                dma((count,)), dma,
                dma((2, count)), dma((2, count)), dma((2, count)), dma((2, count)), dma((2, count)), dma((2, count)),
            ],
            compiler_params=pltpu.CompilerParams(collective_id=0, has_side_effects=True, vmem_limit_bytes=60 * 1024 * 1024),
            name='block_lasso',
        )(x_local, coef_local.T, targets_local.T, step_local[None, :])
        return w_t.T, r_t.T

    return jax.shard_map(local_run, mesh=mesh, in_specs=(P('prob', 'feat'), P(('prob', 'feat'), None), P('prob', None), P(('prob', 'feat'))), out_specs=(P(('prob', 'feat'), None), P('prob', None)), check_vma=False)
```

```python
import functools

import jax
import jax.numpy as jnp
from jax import lax
from jax.experimental import pallas as pl
from jax.experimental.pallas import tpu as pltpu
from jax.sharding import PartitionSpec as P

SWEEPS = 6
COMBINE_WEIGHT = 0.8
LAG = 2
IN_FLIGHT = 2
TILE = 256
MESH = pl.DeviceIdType.MESH
OWN, PARTNER, CROSS, RELAYED = 0, 1, 2, 3


def chunk_list(samples):
    size = samples // 8
    return [(i * size, size) for i in range(8)]


def kernel(chunks, lasso_weight, samples, *refs):
    (x_hbm, w0_ref, y_hbm, eta_ref, wv, rv, xv, xt, ubuf, dwv, x_sem, y_sem,
     own_send, cross_send, relay_send, own_recv, cross_recv, relay_recv) = refs
    count = len(chunks)
    targets = w0_ref.shape[0]
    me = lax.axis_index('feat')
    partner = me + 1 - 2 * lax.rem(me, 2)
    cross = 3 - me

    def rows_of(c):
        start, size = chunks[c]
        return pl.ds(start, size)

    def tiles_of(c):
        start, size = chunks[c]
        return range(start // TILE, (start + size) // TILE)

    def x_copy(c):
        return pltpu.make_async_copy(x_hbm.at[rows_of(c)], xv.at[rows_of(c)], x_sem.at[c])

    def remote(par, c, src, dst, peer, send_sem, recv_sem):
        return pltpu.make_async_remote_copy(
            src_ref=ubuf.at[par, src, :, rows_of(c)], dst_ref=ubuf.at[par, dst, :, rows_of(c)],
            send_sem=send_sem.at[par, c], recv_sem=recv_sem.at[par, c], device_id={'feat': peer}, device_id_type=MESH)

    def own_copy(par, c):
        return remote(par, c, OWN, PARTNER, partner, own_send, own_recv)

    def cross_copy(par, c):
        return remote(par, c, OWN, CROSS, cross, cross_send, cross_recv)

    def relay_copy(par, c):
        return remote(par, c, CROSS, RELAYED, partner, relay_send, relay_recv)

    def forward(par, c, first):
        change = dwv[...]
        for t in tiles_of(c):
            rows = pl.ds(t * TILE, TILE)
            if first:
                product = lax.dot_general(change, xv[rows, :], (((1,), (1,)), ((), ())), preferred_element_type=jnp.float32)
                xt[t] = xv[rows, :].T
            else:
                product = jnp.dot(change, xt[t], preferred_element_type=jnp.float32)
            ubuf[par, OWN, :, rows] = product.astype(jnp.bfloat16)

    def update_weights(gradient):
        eta = jnp.broadcast_to(eta_ref[...], gradient.shape)
        threshold = eta * lasso_weight
        weights = wv[...]
        stepped = weights + eta * (gradient * (1.0 / samples))
        shrunk = jnp.where(stepped > threshold, stepped - threshold, jnp.where(stepped < -threshold, stepped + threshold, 0.0))
        change = shrunk - weights
        wv[...] = weights + COMBINE_WEIGHT * change
        dwv[...] = change.astype(jnp.bfloat16)

    def wait_sends(par):
        for c in range(count):
            own_copy(par, c).wait_send()
            if c >= count - IN_FLIGHT:
                cross_copy(par, c).wait_send()
            relay_copy(par, c).wait_send()

    def phase(par, first=False, last=False):
        for c in range(count):
            if first:
                x_copy(c).wait()
            forward(par, c, first)
            if c == count // 2 and not first:
                wait_sends(1 - par)
            if c >= IN_FLIGHT:
                cross_copy(par, c - IN_FLIGHT).wait_send()
            cross_copy(par, c).start()
            own_copy(par, c).start()
        if first:
            pltpu.make_async_copy(y_hbm, rv, y_sem).wait()
        gradient = None
        for step in range(count + LAG):
            if step < count:
                cross_copy(par, step).wait_recv()
                relay_copy(par, step).start()
            c = step - LAG
            if c < 0:
                continue
            own_copy(par, c).wait_recv()
            relay_copy(par, c).wait_recv()
            rows = rows_of(c)
            u = [ubuf[par, slot, :, rows].astype(jnp.float32) for slot in range(4)]
            total = (u[OWN] + u[PARTNER]) + (u[CROSS] + u[RELAYED])
            residual = rv[:, rows] - (total if first else COMBINE_WEIGHT * total)
            rv[:, rows] = residual
            if not last:
                part = jnp.dot(residual.astype(jnp.bfloat16), xv[rows, :], preferred_element_type=jnp.float32)
                gradient = part if gradient is None else gradient + part
        if not last:
            update_weights(gradient)

    for c in range(count):
        x_copy(c).start()
        if c == 0:
            pltpu.make_async_copy(y_hbm, rv, y_sem).start()
    barrier = pltpu.get_barrier_semaphore()
    for peer in (partner, cross):
        pl.semaphore_signal(barrier, inc=1, device_id={'feat': peer}, device_id_type=MESH)
    wv[...] = w0_ref[...]
    dwv[...] = w0_ref[...].astype(jnp.bfloat16)
    pl.semaphore_wait(barrier, 2)

    phase(0, first=True)

    def sweep(s, carry):
        phase(lax.rem(s, 2))
        return carry

    lax.fori_loop(1, SWEEPS, sweep, 0)
    phase(SWEEPS % 2, last=True)
    wait_sends(SWEEPS % 2)


def solution(mesh):
    group_size = mesh.shape['feat']

    def local_run(x_local, coef_local, targets_local, step_local):
        samples, local_features = x_local.shape
        targets = coef_local.shape[1]
        features = local_features * group_size
        lasso_weight = 0.3 * group_size / features ** 0.5
        chunks = chunk_list(samples)
        count = len(chunks)
        any_spec = pl.BlockSpec(memory_space=pl.ANY)
        vmem_spec = pl.BlockSpec(memory_space=pltpu.VMEM)
        dma = pltpu.SemaphoreType.DMA
        w_t, r_t = pl.pallas_call(
            functools.partial(kernel, chunks, lasso_weight, samples),
            out_shape=(pltpu.VMEM((targets, local_features), jnp.float32), pltpu.VMEM((targets, samples), jnp.float32)),
            in_specs=[pl.BlockSpec(memory_space=pltpu.HBM), vmem_spec, pl.BlockSpec(memory_space=pltpu.HBM), vmem_spec],
            out_specs=(vmem_spec, vmem_spec),
            scratch_shapes=[
                pltpu.VMEM((samples, local_features), jnp.bfloat16),
                pltpu.VMEM((samples // TILE, local_features, TILE), jnp.bfloat16),
                pltpu.VMEM((2, 4, targets, samples), jnp.bfloat16),
                pltpu.VMEM((targets, local_features), jnp.bfloat16),
                dma((count,)), dma,
                dma((2, count)), dma((2, count)), dma((2, count)), dma((2, count)), dma((2, count)), dma((2, count)),
            ],
            compiler_params=pltpu.CompilerParams(collective_id=0, has_side_effects=True, vmem_limit_bytes=60 * 1024 * 1024),
            name='block_lasso',
        )(x_local, coef_local.T, targets_local.T, step_local[None, :])
        return w_t.T, r_t.T

    return jax.shard_map(local_run, mesh=mesh, in_specs=(P('prob', 'feat'), P(('prob', 'feat'), None), P('prob', None), P(('prob', 'feat'))), out_specs=(P(('prob', 'feat'), None), P('prob', None)), check_vma=False)
```

```python
import functools

import jax
import jax.numpy as jnp
from jax import lax
from jax.experimental import pallas as pl
from jax.experimental.pallas import tpu as pltpu
from jax.sharding import PartitionSpec as P

SWEEPS = 6
COMBINE_WEIGHT = 0.8
LAG = 2
TILE = 256
MESH = pl.DeviceIdType.MESH
OWN, PARTNER, CROSS, RELAYED = 0, 1, 2, 3


def chunk_list(samples):
    size = samples // 8
    return [(i * size, size) for i in range(8)]


def kernel(chunks, lasso_weight, samples, *refs):
    (x_hbm, w0_ref, y_hbm, eta_ref, wv, rv, xv, xt, ubuf, dwv, x_sem, y_sem,
     own_send, cross_send, relay_send, own_recv, cross_recv, relay_recv) = refs
    count = len(chunks)
    targets = w0_ref.shape[0]
    me = lax.axis_index('feat')
    partner = me + 1 - 2 * lax.rem(me, 2)
    cross = 3 - me

    def rows_of(c):
        start, size = chunks[c]
        return pl.ds(start, size)

    def tiles_of(c):
        start, size = chunks[c]
        return range(start // TILE, (start + size) // TILE)

    def x_copy(c, half):
        start, size = chunks[c]
        rows = pl.ds(start + half * (size // 2), size // 2)
        return pltpu.make_async_copy(x_hbm.at[rows], xv.at[rows], x_sem.at[c, half])

    def remote(par, c, src, dst, peer, send_sem, recv_sem):
        return pltpu.make_async_remote_copy(
            src_ref=ubuf.at[par, src, :, rows_of(c)], dst_ref=ubuf.at[par, dst, :, rows_of(c)],
            send_sem=send_sem.at[par, c], recv_sem=recv_sem.at[par, c], device_id={'feat': peer}, device_id_type=MESH)

    def own_copy(par, c):
        return remote(par, c, OWN, PARTNER, partner, own_send, own_recv)

    def cross_copy(par, c):
        return remote(par, c, OWN, CROSS, cross, cross_send, cross_recv)

    def relay_copy(par, c):
        return remote(par, c, CROSS, RELAYED, partner, relay_send, relay_recv)

    def forward(par, c, first):
        change = dwv[...]
        for i, t in enumerate(tiles_of(c)):
            rows = pl.ds(t * TILE, TILE)
            if first and 2 * i % len(tiles_of(c)) == 0:
                x_copy(c, 2 * i // len(tiles_of(c))).wait()
            if first:
                product = lax.dot_general(change, xv[rows, :], (((1,), (1,)), ((), ())), preferred_element_type=jnp.float32)
                xt[t] = xv[rows, :].T
            else:
                product = jnp.dot(change, xt[t], preferred_element_type=jnp.float32)
            ubuf[par, OWN, :, rows] = product.astype(jnp.bfloat16)

    def update_weights(gradient):
        eta = jnp.broadcast_to(eta_ref[...], gradient.shape)
        threshold = eta * lasso_weight
        weights = wv[...]
        stepped = weights + eta * (gradient * (1.0 / samples))
        shrunk = jnp.where(stepped > threshold, stepped - threshold, jnp.where(stepped < -threshold, stepped + threshold, 0.0))
        change = shrunk - weights
        wv[...] = weights + COMBINE_WEIGHT * change
        dwv[...] = change.astype(jnp.bfloat16)

    def wait_sends(par):
        for c in range(count):
            own_copy(par, c).wait_send()
            cross_copy(par, c).wait_send()
            relay_copy(par, c).wait_send()

    def phase(par, first=False, last=False):
        for c in range(count):
            forward(par, c, first)
            if c == count // 2 and not first:
                wait_sends(1 - par)
            cross_copy(par, c).start()
            own_copy(par, c).start()
        if first:
            pltpu.make_async_copy(y_hbm, rv, y_sem).wait()
        gradient = None
        for step in range(count + LAG):
            if step < count:
                cross_copy(par, step).wait_recv()
                relay_copy(par, step).start()
            c = step - LAG
            if c < 0:
                continue
            own_copy(par, c).wait_recv()
            relay_copy(par, c).wait_recv()
            rows = rows_of(c)
            u = [ubuf[par, slot, :, rows].astype(jnp.float32) for slot in range(4)]
            total = (u[OWN] + u[PARTNER]) + (u[CROSS] + u[RELAYED])
            residual = rv[:, rows] - (total if first else COMBINE_WEIGHT * total)
            rv[:, rows] = residual
            if not last:
                part = jnp.dot(residual.astype(jnp.bfloat16), xv[rows, :], preferred_element_type=jnp.float32)
                gradient = part if gradient is None else gradient + part
        if not last:
            update_weights(gradient)

    for c in range(count):
        x_copy(c, 0).start()
        x_copy(c, 1).start()
        if c == 0:
            pltpu.make_async_copy(y_hbm, rv, y_sem).start()
    barrier = pltpu.get_barrier_semaphore()
    for peer in (partner, cross):
        pl.semaphore_signal(barrier, inc=1, device_id={'feat': peer}, device_id_type=MESH)
    wv[...] = w0_ref[...]
    dwv[...] = w0_ref[...].astype(jnp.bfloat16)
    pl.semaphore_wait(barrier, 2)

    phase(0, first=True)

    def sweep(s, carry):
        phase(lax.rem(s, 2))
        return carry

    lax.fori_loop(1, SWEEPS, sweep, 0)
    phase(SWEEPS % 2, last=True)
    wait_sends(SWEEPS % 2)


def leave(w_ref, r_ref, w_hbm, r_hbm, sem):
    copies = [pltpu.make_async_copy(r_ref, r_hbm, sem.at[1]), pltpu.make_async_copy(w_ref, w_hbm, sem.at[0])]
    for copy in copies:
        copy.start()
    for copy in copies:
        copy.wait()


def solution(mesh):
    group_size = mesh.shape['feat']

    def local_run(x_local, coef_local, targets_local, step_local):
        samples, local_features = x_local.shape
        targets = coef_local.shape[1]
        features = local_features * group_size
        lasso_weight = 0.3 * group_size / features ** 0.5
        chunks = chunk_list(samples)
        count = len(chunks)
        any_spec = pl.BlockSpec(memory_space=pl.ANY)
        vmem_spec = pl.BlockSpec(memory_space=pltpu.VMEM)
        dma = pltpu.SemaphoreType.DMA
        w_t, r_t = pl.pallas_call(
            functools.partial(kernel, chunks, lasso_weight, samples),
            out_shape=(pltpu.VMEM((targets, local_features), jnp.float32), pltpu.VMEM((targets, samples), jnp.float32)),
            in_specs=[pl.BlockSpec(memory_space=pltpu.HBM), vmem_spec, pl.BlockSpec(memory_space=pltpu.HBM), vmem_spec],
            out_specs=(vmem_spec, vmem_spec),
            scratch_shapes=[
                pltpu.VMEM((samples, local_features), jnp.bfloat16),
                pltpu.VMEM((samples // TILE, local_features, TILE), jnp.bfloat16),
                pltpu.VMEM((2, 4, targets, samples), jnp.bfloat16),
                pltpu.VMEM((targets, local_features), jnp.bfloat16),
                dma((count, 2)), dma,
                dma((2, count)), dma((2, count)), dma((2, count)), dma((2, count)), dma((2, count)), dma((2, count)),
            ],
            compiler_params=pltpu.CompilerParams(collective_id=0, has_side_effects=True, vmem_limit_bytes=60 * 1024 * 1024),
            name='block_lasso',
        )(x_local, coef_local.T, targets_local.T, step_local[None, :])
        w_t, r_t = pl.pallas_call(
            leave,
            out_shape=(jax.ShapeDtypeStruct(w_t.shape, w_t.dtype), jax.ShapeDtypeStruct(r_t.shape, r_t.dtype)),
            in_specs=[vmem_spec, vmem_spec],
            out_specs=(any_spec, any_spec),
            scratch_shapes=[dma((2,))],
            name='leave',
        )(pltpu.with_memory_space_constraint(w_t, pltpu.VMEM), pltpu.with_memory_space_constraint(r_t, pltpu.VMEM))
        return w_t.T, r_t.T

    return jax.shard_map(local_run, mesh=mesh, in_specs=(P('prob', 'feat'), P(('prob', 'feat'), None), P('prob', None), P(('prob', 'feat'))), out_specs=(P(('prob', 'feat'), None), P('prob', None)), check_vma=False)
```

```python
import functools

import jax
import jax.numpy as jnp
from jax import lax
from jax.experimental import pallas as pl
from jax.experimental.pallas import tpu as pltpu
from jax.sharding import PartitionSpec as P

SWEEPS = 6
COMBINE_WEIGHT = 0.8
LAG = 2
TILE = 256
MESH = pl.DeviceIdType.MESH
OWN, PARTNER, CROSS, RELAYED = 0, 1, 2, 3


def chunk_list(samples):
    size = samples // 8
    return [(i * size, size) for i in range(8)]


def kernel(chunks, lasso_weight, samples, *refs):
    (x_hbm, w0_ref, y_hbm, eta_ref, wv, rv, xv, xt, ubuf, dwv, x_sem, y_sem,
     own_send, cross_send, relay_send, own_recv, cross_recv, relay_recv) = refs
    count = len(chunks)
    targets = w0_ref.shape[0]
    me = lax.axis_index('feat')
    partner = me + 1 - 2 * lax.rem(me, 2)
    cross = 3 - me

    def rows_of(c):
        start, size = chunks[c]
        return pl.ds(start, size)

    def tiles_of(c):
        start, size = chunks[c]
        return range(start // TILE, (start + size) // TILE)

    def x_copy(c):
        return pltpu.make_async_copy(x_hbm.at[rows_of(c)], xv.at[rows_of(c)], x_sem.at[c])

    def remote(par, c, src, dst, peer, send_sem, recv_sem):
        return pltpu.make_async_remote_copy(
            src_ref=ubuf.at[par, src, :, rows_of(c)], dst_ref=ubuf.at[par, dst, :, rows_of(c)],
            send_sem=send_sem.at[par, c], recv_sem=recv_sem.at[par, c], device_id={'feat': peer}, device_id_type=MESH)

    def own_copy(par, c):
        return remote(par, c, OWN, PARTNER, partner, own_send, own_recv)

    def cross_copy(par, c):
        return remote(par, c, OWN, CROSS, cross, cross_send, cross_recv)

    def relay_copy(par, c):
        return remote(par, c, CROSS, RELAYED, partner, relay_send, relay_recv)

    def forward(par, c, first):
        change = dwv[...]
        for t in tiles_of(c):
            rows = pl.ds(t * TILE, TILE)
            if first:
                product = lax.dot_general(change, xv[rows, :], (((1,), (1,)), ((), ())), preferred_element_type=jnp.float32)
                xt[t] = xv[rows, :].T
            else:
                product = jnp.dot(change, xt[t], preferred_element_type=jnp.float32)
            ubuf[par, OWN, :, rows] = product.astype(jnp.bfloat16)

    def update_weights(gradient):
        eta = jnp.broadcast_to(eta_ref[...], gradient.shape)
        threshold = eta * lasso_weight
        weights = wv[...]
        stepped = weights + eta * (gradient * (1.0 / samples))
        shrunk = jnp.where(stepped > threshold, stepped - threshold, jnp.where(stepped < -threshold, stepped + threshold, 0.0))
        change = shrunk - weights
        wv[...] = weights + COMBINE_WEIGHT * change
        dwv[...] = change.astype(jnp.bfloat16)

    def wait_sends(par):
        for c in range(count):
            own_copy(par, c).wait_send()
            cross_copy(par, c).wait_send()
            relay_copy(par, c).wait_send()

    def phase(par, first=False, last=False):
        for c in range(count):
            if first:
                x_copy(c).wait()
            forward(par, c, first)
            if c == count // 2 and not first:
                wait_sends(1 - par)
            cross_copy(par, c).start()
            own_copy(par, c).start()
        if first:
            pltpu.make_async_copy(y_hbm, rv, y_sem).wait()
        gradient = None
        for step in range(count + LAG):
            if step < count:
                cross_copy(par, step).wait_recv()
                relay_copy(par, step).start()
            c = step - LAG
            if c < 0:
                continue
            own_copy(par, c).wait_recv()
            relay_copy(par, c).wait_recv()
            rows = rows_of(c)
            u = [ubuf[par, slot, :, rows].astype(jnp.float32) for slot in range(4)]
            total = (u[OWN] + u[PARTNER]) + (u[CROSS] + u[RELAYED])
            residual = rv[:, rows] - (total if first else COMBINE_WEIGHT * total)
            rv[:, rows] = residual
            if not last:
                part = jnp.dot(residual.astype(jnp.bfloat16), xv[rows, :], preferred_element_type=jnp.float32)
                gradient = part if gradient is None else gradient + part
        if not last:
            update_weights(gradient)

    for c in range(count):
        x_copy(c).start()
        if c == 0:
            pltpu.make_async_copy(y_hbm, rv, y_sem).start()
    barrier = pltpu.get_barrier_semaphore()
    for peer in (partner, cross):
        pl.semaphore_signal(barrier, inc=1, device_id={'feat': peer}, device_id_type=MESH)
    wv[...] = w0_ref[...]
    dwv[...] = w0_ref[...].astype(jnp.bfloat16)
    pl.semaphore_wait(barrier, 2)

    phase(0, first=True)

    def sweep(s, carry):
        phase(lax.rem(s, 2))
        return carry

    lax.fori_loop(1, SWEEPS, sweep, 0)
    phase(SWEEPS % 2, last=True)
    wait_sends(SWEEPS % 2)


def leave(w_ref, r_ref, w_hbm, r_hbm, sem):
    copies = [pltpu.make_async_copy(r_ref, r_hbm, sem.at[1]), pltpu.make_async_copy(w_ref, w_hbm, sem.at[0])]
    for copy in copies:
        copy.start()
    for copy in copies:
        copy.wait()


def solution(mesh):
    group_size = mesh.shape['feat']

    def local_run(x_local, coef_local, targets_local, step_local):
        samples, local_features = x_local.shape
        targets = coef_local.shape[1]
        features = local_features * group_size
        lasso_weight = 0.3 * group_size / features ** 0.5
        chunks = chunk_list(samples)
        count = len(chunks)
        any_spec = pl.BlockSpec(memory_space=pl.ANY)
        vmem_spec = pl.BlockSpec(memory_space=pltpu.VMEM)
        dma = pltpu.SemaphoreType.DMA
        w_t, r_t = pl.pallas_call(
            functools.partial(kernel, chunks, lasso_weight, samples),
            out_shape=(pltpu.VMEM((targets, local_features), jnp.float32), pltpu.VMEM((targets, samples), jnp.float32)),
            in_specs=[pl.BlockSpec(memory_space=pltpu.HBM), vmem_spec, pl.BlockSpec(memory_space=pltpu.HBM), vmem_spec],
            out_specs=(vmem_spec, vmem_spec),
            scratch_shapes=[
                pltpu.VMEM((samples, local_features), jnp.bfloat16),
                pltpu.VMEM((samples // TILE, local_features, TILE), jnp.bfloat16),
                pltpu.VMEM((2, 4, targets, samples), jnp.bfloat16),
                pltpu.VMEM((targets, local_features), jnp.bfloat16),
                dma((count,)), dma,
                dma((2, count)), dma((2, count)), dma((2, count)), dma((2, count)), dma((2, count)), dma((2, count)),
            ],
            compiler_params=pltpu.CompilerParams(collective_id=0, has_side_effects=True, vmem_limit_bytes=60 * 1024 * 1024),
            name='block_lasso',
        )(x_local, coef_local.T, targets_local.T, step_local[None, :])
        w_t, r_t = pl.pallas_call(
            leave,
            out_shape=(jax.ShapeDtypeStruct(w_t.shape, w_t.dtype), jax.ShapeDtypeStruct(r_t.shape, r_t.dtype)),
            in_specs=[vmem_spec, vmem_spec],
            out_specs=(any_spec, any_spec),
            scratch_shapes=[dma((2,))],
            name='leave',
        )(pltpu.with_memory_space_constraint(w_t, pltpu.VMEM), pltpu.with_memory_space_constraint(r_t, pltpu.VMEM))
        return w_t.T, r_t.T

    return jax.shard_map(local_run, mesh=mesh, in_specs=(P('prob', 'feat'), P(('prob', 'feat'), None), P('prob', None), P(('prob', 'feat'))), out_specs=(P(('prob', 'feat'), None), P('prob', None)), check_vma=False)
```

```python
import functools

import jax
import jax.numpy as jnp
from jax import lax
from jax.experimental import pallas as pl
from jax.experimental.pallas import tpu as pltpu
from jax.sharding import PartitionSpec as P

SWEEPS = 6
COMBINE_WEIGHT = 0.8
LAG = 2
TILE = 256
MESH = pl.DeviceIdType.MESH
OWN, PARTNER, CROSS, RELAYED = 0, 1, 2, 3


def chunk_list(samples):
    sizes = [1024, 1024] + [2048] * (samples // 2048 - 1)
    return [(sum(sizes[:i]), size) for i, size in enumerate(sizes)]


def kernel(chunks, lasso_weight, samples, *refs):
    (x_hbm, w0_ref, y_hbm, eta_ref, wv, rv, xv, xt, ubuf, dwv, x_sem, y_sem,
     own_send, cross_send, relay_send, own_recv, cross_recv, relay_recv) = refs
    count = len(chunks)
    targets = w0_ref.shape[0]
    me = lax.axis_index('feat')
    partner = me + 1 - 2 * lax.rem(me, 2)
    cross = 3 - me

    def rows_of(c):
        start, size = chunks[c]
        return pl.ds(start, size)

    def tiles_of(c):
        start, size = chunks[c]
        return range(start // TILE, (start + size) // TILE)

    def x_copy(c):
        return pltpu.make_async_copy(x_hbm.at[rows_of(c)], xv.at[rows_of(c)], x_sem.at[c])

    def remote(par, c, src, dst, peer, send_sem, recv_sem):
        return pltpu.make_async_remote_copy(
            src_ref=ubuf.at[par, src, :, rows_of(c)], dst_ref=ubuf.at[par, dst, :, rows_of(c)],
            send_sem=send_sem.at[par, c], recv_sem=recv_sem.at[par, c], device_id={'feat': peer}, device_id_type=MESH)

    def own_copy(par, c):
        return remote(par, c, OWN, PARTNER, partner, own_send, own_recv)

    def cross_copy(par, c):
        return remote(par, c, OWN, CROSS, cross, cross_send, cross_recv)

    def relay_copy(par, c):
        return remote(par, c, CROSS, RELAYED, partner, relay_send, relay_recv)

    def forward(par, c, first):
        change = dwv[...]
        for t in tiles_of(c):
            rows = pl.ds(t * TILE, TILE)
            if first:
                product = lax.dot_general(change, xv[rows, :], (((1,), (1,)), ((), ())), preferred_element_type=jnp.float32)
                xt[t] = xv[rows, :].T
            else:
                product = jnp.dot(change, xt[t], preferred_element_type=jnp.float32)
            ubuf[par, OWN, :, rows] = product.astype(jnp.bfloat16)

    def update_weights(gradient):
        eta = jnp.broadcast_to(eta_ref[...], gradient.shape)
        threshold = eta * lasso_weight
        weights = wv[...]
        stepped = weights + eta * (gradient * (1.0 / samples))
        shrunk = jnp.where(stepped > threshold, stepped - threshold, jnp.where(stepped < -threshold, stepped + threshold, 0.0))
        change = shrunk - weights
        wv[...] = weights + COMBINE_WEIGHT * change
        dwv[...] = change.astype(jnp.bfloat16)

    def wait_sends(par):
        for c in range(count):
            own_copy(par, c).wait_send()
            cross_copy(par, c).wait_send()
            relay_copy(par, c).wait_send()

    def phase(par, first=False, last=False):
        for c in range(count):
            if first:
                x_copy(c).wait()
            forward(par, c, first)
            if c == count // 2 and not first:
                wait_sends(1 - par)
            cross_copy(par, c).start()
            own_copy(par, c).start()
        if first:
            pltpu.make_async_copy(y_hbm, rv, y_sem).wait()
        gradient = None
        for step in range(count + LAG):
            if step < count:
                cross_copy(par, step).wait_recv()
                relay_copy(par, step).start()
            c = step - LAG
            if c < 0:
                continue
            own_copy(par, c).wait_recv()
            relay_copy(par, c).wait_recv()
            rows = rows_of(c)
            u = [ubuf[par, slot, :, rows].astype(jnp.float32) for slot in range(4)]
            total = (u[OWN] + u[PARTNER]) + (u[CROSS] + u[RELAYED])
            residual = rv[:, rows] - (total if first else COMBINE_WEIGHT * total)
            rv[:, rows] = residual
            if not last:
                part = jnp.dot(residual.astype(jnp.bfloat16), xv[rows, :], preferred_element_type=jnp.float32)
                gradient = part if gradient is None else gradient + part
        if not last:
            update_weights(gradient)

    for c in range(count):
        x_copy(c).start()
        if c == 0:
            pltpu.make_async_copy(y_hbm, rv, y_sem).start()
    barrier = pltpu.get_barrier_semaphore()
    for peer in (partner, cross):
        pl.semaphore_signal(barrier, inc=1, device_id={'feat': peer}, device_id_type=MESH)
    wv[...] = w0_ref[...]
    dwv[...] = w0_ref[...].astype(jnp.bfloat16)
    pl.semaphore_wait(barrier, 2)

    phase(0, first=True)

    def sweep(s, carry):
        phase(lax.rem(s, 2))
        return carry

    lax.fori_loop(1, SWEEPS, sweep, 0)
    phase(SWEEPS % 2, last=True)
    wait_sends(SWEEPS % 2)


def leave(w_ref, r_ref, w_hbm, r_hbm, sem):
    copies = [pltpu.make_async_copy(r_ref, r_hbm, sem.at[1]), pltpu.make_async_copy(w_ref, w_hbm, sem.at[0])]
    for copy in copies:
        copy.start()
    for copy in copies:
        copy.wait()


def solution(mesh):
    group_size = mesh.shape['feat']

    def local_run(x_local, coef_local, targets_local, step_local):
        samples, local_features = x_local.shape
        targets = coef_local.shape[1]
        features = local_features * group_size
        lasso_weight = 0.3 * group_size / features ** 0.5
        chunks = chunk_list(samples)
        count = len(chunks)
        any_spec = pl.BlockSpec(memory_space=pl.ANY)
        vmem_spec = pl.BlockSpec(memory_space=pltpu.VMEM)
        dma = pltpu.SemaphoreType.DMA
        w_t, r_t = pl.pallas_call(
            functools.partial(kernel, chunks, lasso_weight, samples),
            out_shape=(pltpu.VMEM((targets, local_features), jnp.float32), pltpu.VMEM((targets, samples), jnp.float32)),
            in_specs=[pl.BlockSpec(memory_space=pltpu.HBM), vmem_spec, pl.BlockSpec(memory_space=pltpu.HBM), vmem_spec],
            out_specs=(vmem_spec, vmem_spec),
            scratch_shapes=[
                pltpu.VMEM((samples, local_features), jnp.bfloat16),
                pltpu.VMEM((samples // TILE, local_features, TILE), jnp.bfloat16),
                pltpu.VMEM((2, 4, targets, samples), jnp.bfloat16),
                pltpu.VMEM((targets, local_features), jnp.bfloat16),
                dma((count,)), dma,
                dma((2, count)), dma((2, count)), dma((2, count)), dma((2, count)), dma((2, count)), dma((2, count)),
            ],
            compiler_params=pltpu.CompilerParams(collective_id=0, has_side_effects=True, vmem_limit_bytes=60 * 1024 * 1024),
            name='block_lasso',
        )(x_local, coef_local.T, targets_local.T, step_local[None, :])
        w_t, r_t = pl.pallas_call(
            leave,
            out_shape=(jax.ShapeDtypeStruct(w_t.shape, w_t.dtype), jax.ShapeDtypeStruct(r_t.shape, r_t.dtype)),
            in_specs=[vmem_spec, vmem_spec],
            out_specs=(any_spec, any_spec),
            scratch_shapes=[dma((2,))],
            name='leave',
        )(pltpu.with_memory_space_constraint(w_t, pltpu.VMEM), pltpu.with_memory_space_constraint(r_t, pltpu.VMEM))
        return w_t.T, r_t.T

    return jax.shard_map(local_run, mesh=mesh, in_specs=(P('prob', 'feat'), P(('prob', 'feat'), None), P('prob', None), P(('prob', 'feat'))), out_specs=(P(('prob', 'feat'), None), P('prob', None)), check_vma=False)
```

```python
import functools

import jax
import jax.numpy as jnp
from jax import lax
from jax.experimental import pallas as pl
from jax.experimental.pallas import tpu as pltpu
from jax.sharding import PartitionSpec as P

SWEEPS = 6
COMBINE_WEIGHT = 0.8
LAG = 2
TILE = 256
MESH = pl.DeviceIdType.MESH
OWN, PARTNER, CROSS, RELAYED = 0, 1, 2, 3


def chunk_list(samples):
    sizes = [2048] + [3072] * ((samples - 4096) // 3072) + [2048]
    return [(sum(sizes[:i]), size) for i, size in enumerate(sizes)]


def kernel(chunks, lasso_weight, samples, *refs):
    (x_hbm, w0_ref, y_hbm, eta_ref, wv, rv, xv, xt, ubuf, dwv, x_sem, y_sem,
     own_send, cross_send, relay_send, own_recv, cross_recv, relay_recv) = refs
    count = len(chunks)
    targets = w0_ref.shape[0]
    me = lax.axis_index('feat')
    partner = me + 1 - 2 * lax.rem(me, 2)
    cross = 3 - me

    def rows_of(c):
        start, size = chunks[c]
        return pl.ds(start, size)

    def tiles_of(c):
        start, size = chunks[c]
        return range(start // TILE, (start + size) // TILE)

    def x_copy(c):
        return pltpu.make_async_copy(x_hbm.at[rows_of(c)], xv.at[rows_of(c)], x_sem.at[c])

    def remote(par, c, src, dst, peer, send_sem, recv_sem):
        return pltpu.make_async_remote_copy(
            src_ref=ubuf.at[par, src, :, rows_of(c)], dst_ref=ubuf.at[par, dst, :, rows_of(c)],
            send_sem=send_sem.at[par, c], recv_sem=recv_sem.at[par, c], device_id={'feat': peer}, device_id_type=MESH)

    def own_copy(par, c):
        return remote(par, c, OWN, PARTNER, partner, own_send, own_recv)

    def cross_copy(par, c):
        return remote(par, c, OWN, CROSS, cross, cross_send, cross_recv)

    def relay_copy(par, c):
        return remote(par, c, CROSS, RELAYED, partner, relay_send, relay_recv)

    def forward(par, c, first):
        change = dwv[...]
        for t in tiles_of(c):
            rows = pl.ds(t * TILE, TILE)
            if first:
                product = lax.dot_general(change, xv[rows, :], (((1,), (1,)), ((), ())), preferred_element_type=jnp.float32)
                xt[t] = xv[rows, :].T
            else:
                product = jnp.dot(change, xt[t], preferred_element_type=jnp.float32)
            ubuf[par, OWN, :, rows] = product.astype(jnp.bfloat16)

    def update_weights(gradient):
        eta = jnp.broadcast_to(eta_ref[...], gradient.shape)
        threshold = eta * lasso_weight
        weights = wv[...]
        stepped = weights + eta * (gradient * (1.0 / samples))
        shrunk = jnp.where(stepped > threshold, stepped - threshold, jnp.where(stepped < -threshold, stepped + threshold, 0.0))
        change = shrunk - weights
        wv[...] = weights + COMBINE_WEIGHT * change
        dwv[...] = change.astype(jnp.bfloat16)

    def wait_sends(par):
        for c in range(count):
            own_copy(par, c).wait_send()
            cross_copy(par, c).wait_send()
            relay_copy(par, c).wait_send()

    def phase(par, first=False, last=False):
        for c in range(count):
            if first:
                x_copy(c).wait()
            forward(par, c, first)
            if c == count // 2 and not first:
                wait_sends(1 - par)
            cross_copy(par, c).start()
            own_copy(par, c).start()
        if first:
            pltpu.make_async_copy(y_hbm, rv, y_sem).wait()
        gradient = None
        for step in range(count + LAG):
            if step < count:
                cross_copy(par, step).wait_recv()
                relay_copy(par, step).start()
            c = step - LAG
            if c < 0:
                continue
            own_copy(par, c).wait_recv()
            relay_copy(par, c).wait_recv()
            rows = rows_of(c)
            u = [ubuf[par, slot, :, rows].astype(jnp.float32) for slot in range(4)]
            total = (u[OWN] + u[PARTNER]) + (u[CROSS] + u[RELAYED])
            residual = rv[:, rows] - (total if first else COMBINE_WEIGHT * total)
            rv[:, rows] = residual
            if not last:
                part = jnp.dot(residual.astype(jnp.bfloat16), xv[rows, :], preferred_element_type=jnp.float32)
                gradient = part if gradient is None else gradient + part
        if not last:
            update_weights(gradient)

    for c in range(count):
        x_copy(c).start()
        if c == 0:
            pltpu.make_async_copy(y_hbm, rv, y_sem).start()
    barrier = pltpu.get_barrier_semaphore()
    for peer in (partner, cross):
        pl.semaphore_signal(barrier, inc=1, device_id={'feat': peer}, device_id_type=MESH)
    wv[...] = w0_ref[...]
    dwv[...] = w0_ref[...].astype(jnp.bfloat16)
    pl.semaphore_wait(barrier, 2)

    phase(0, first=True)

    def sweep(s, carry):
        phase(lax.rem(s, 2))
        return carry

    lax.fori_loop(1, SWEEPS, sweep, 0)
    phase(SWEEPS % 2, last=True)
    wait_sends(SWEEPS % 2)


def leave(w_ref, r_ref, w_hbm, r_hbm, sem):
    copies = [pltpu.make_async_copy(r_ref, r_hbm, sem.at[1]), pltpu.make_async_copy(w_ref, w_hbm, sem.at[0])]
    for copy in copies:
        copy.start()
    for copy in copies:
        copy.wait()


def solution(mesh):
    group_size = mesh.shape['feat']

    def local_run(x_local, coef_local, targets_local, step_local):
        samples, local_features = x_local.shape
        targets = coef_local.shape[1]
        features = local_features * group_size
        lasso_weight = 0.3 * group_size / features ** 0.5
        chunks = chunk_list(samples)
        count = len(chunks)
        any_spec = pl.BlockSpec(memory_space=pl.ANY)
        vmem_spec = pl.BlockSpec(memory_space=pltpu.VMEM)
        dma = pltpu.SemaphoreType.DMA
        w_t, r_t = pl.pallas_call(
            functools.partial(kernel, chunks, lasso_weight, samples),
            out_shape=(pltpu.VMEM((targets, local_features), jnp.float32), pltpu.VMEM((targets, samples), jnp.float32)),
            in_specs=[pl.BlockSpec(memory_space=pltpu.HBM), vmem_spec, pl.BlockSpec(memory_space=pltpu.HBM), vmem_spec],
            out_specs=(vmem_spec, vmem_spec),
            scratch_shapes=[
                pltpu.VMEM((samples, local_features), jnp.bfloat16),
                pltpu.VMEM((samples // TILE, local_features, TILE), jnp.bfloat16),
                pltpu.VMEM((2, 4, targets, samples), jnp.bfloat16),
                pltpu.VMEM((targets, local_features), jnp.bfloat16),
                dma((count,)), dma,
                dma((2, count)), dma((2, count)), dma((2, count)), dma((2, count)), dma((2, count)), dma((2, count)),
            ],
            compiler_params=pltpu.CompilerParams(collective_id=0, has_side_effects=True, vmem_limit_bytes=60 * 1024 * 1024),
            name='block_lasso',
        )(x_local, coef_local.T, targets_local.T, step_local[None, :])
        w_t, r_t = pl.pallas_call(
            leave,
            out_shape=(jax.ShapeDtypeStruct(w_t.shape, w_t.dtype), jax.ShapeDtypeStruct(r_t.shape, r_t.dtype)),
            in_specs=[vmem_spec, vmem_spec],
            out_specs=(any_spec, any_spec),
            scratch_shapes=[dma((2,))],
            name='leave',
        )(pltpu.with_memory_space_constraint(w_t, pltpu.VMEM), pltpu.with_memory_space_constraint(r_t, pltpu.VMEM))
        return w_t.T, r_t.T

    return jax.shard_map(local_run, mesh=mesh, in_specs=(P('prob', 'feat'), P(('prob', 'feat'), None), P('prob', None), P(('prob', 'feat'))), out_specs=(P(('prob', 'feat'), None), P('prob', None)), check_vma=False)
```
